32 devices in a mesh: rep: 2 (over z, core), dp: 16 (over x, y).
Axes of the slice: x: 4, y: 4, z: 1, core: 2. Of those that a mesh axis runs over, the one named last changes fastest.
The devices are a block of a 4x4x8 slice.
Arguments:
- x: bfloat16 [32, 2048, 768], P(('rep', 'dp')), parts along dimension 0
- dy: bfloat16 [32, 2048, 768], P(('rep', 'dp')), parts along dimension 0
- w_gate: bfloat16 [2, 768, 1792], replicated
- w_up: bfloat16 [2, 768, 1792], replicated
- w_down: bfloat16 [2, 1792, 768], replicated
- m_w_gate: float32 [2, 768, 1792], replicated
- m_w_up: float32 [2, 768, 1792], replicated
- m_w_down: float32 [2, 1792, 768], replicated
- v_w_gate: float32 [2, 768, 1792], replicated
- v_w_up: float32 [2, 768, 1792], replicated
- v_w_down: float32 [2, 1792, 768], replicated
Outputs:
- output 1: bfloat16 [4, 768, 1792], P('rep'), parts along dimension 0
- output 2: bfloat16 [4, 768, 1792], P('rep'), parts along dimension 0
- output 3: bfloat16 [4, 1792, 768], P('rep'), parts along dimension 0
- output 4: float32 [4, 768, 1792], P('rep'), parts along dimension 0
- output 5: float32 [4, 768, 1792], P('rep'), parts along dimension 0
- output 6: float32 [4, 1792, 768], P('rep'), parts along dimension 0
- output 7: float32 [4, 768, 1792], P('rep'), parts along dimension 0
- output 8: float32 [4, 768, 1792], P('rep'), parts along dimension 0
- output 9: float32 [4, 1792, 768], P('rep'), parts along dimension 0
There are 2 independent parts. The reference program is written for one: setup_inputs(seed, part) draws one part's arguments, and reference() takes and returns one part's arrays. A program takes and returns all parts, laid end to end along the dimension named above; an argument that names none is the same for every part.
All inputs are finite; a program needn't handle non-finite values.
Results may differ from the reference program's by a relative error of at most 0.022.
Values are sent between devices in bfloat16 or wider.
A program may use at most 768 MiB of HBM per device.

```python
import jax
import jax.numpy as jnp
from jax import lax

SEQUENCES = 16
TOKENS = 2048
D = 768
FF = 1792
LAYERS = 2
NAMES = ("w_gate", "w_up", "w_down")
SHAPES = {"w_gate": (LAYERS, D, FF), "w_up": (LAYERS, D, FF), "w_down": (LAYERS, FF, D)}


def bump(key, n, height):
    away = (jnp.arange(n, dtype=jnp.int32) - jax.random.randint(key, (), 0, n, jnp.int32)) % n
    return jnp.where(away < n // 8, height, 1.0)


def together(key, own, strength):
    shared = jax.random.normal(key, own.shape[1:], jnp.float32)
    return (own + strength * shared) * lax.rsqrt(1 + strength * strength)


def setup_inputs(seed: int = 0, part: int = 0) -> dict:
    kx, kdy, ka, kb, kz, kf, kh, kl, *keys = jax.random.split(jax.random.key(seed), 8 + 3 * len(NAMES))
    kx, kdy, ka, kb = (jax.random.fold_in(k, part) for k in (kx, kdy, ka, kb))
    kw, km, kv = (keys[i::3] for i in range(3))
    shape = (SEQUENCES, TOKENS, D)
    much_x, much_dy = jax.random.uniform(kz, (2,), jnp.float32, 0.0, 1.0)
    loud = 2.0 ** jax.random.uniform(jax.random.fold_in(kz, 1), (), jnp.float32, -1.0, 2.0)
    layers = 2.0 ** jax.random.uniform(kl, (LAYERS, 1, 1), jnp.float32, -1.0, 1.0)
    x = together(ka, jax.random.normal(kx, shape, jnp.float32), much_x) * bump(kf, D, 4.0)
    dy = together(kb, jax.random.normal(kdy, shape, jnp.float32), much_dy)
    drawn = {"x": x.astype(jnp.bfloat16), "dy": (loud * dy * (SEQUENCES * TOKENS) ** -0.5).astype(jnp.bfloat16)}
    for key, name in zip(kw, NAMES, strict=True):
        w = jax.random.normal(key, SHAPES[name], jnp.float32) * SHAPES[name][1] ** -0.5
        drawn[name] = (w * {"w_gate": 1.0, "w_up": bump(kh, FF, 4.0), "w_down": layers}[name]).astype(jnp.bfloat16)
    for key, name in zip(km, NAMES, strict=True):
        drawn[f"m_{name}"] = 0.1 * jax.random.normal(key, SHAPES[name], jnp.float32)
    for key, name in zip(kv, NAMES, strict=True):
        drawn[f"v_{name}"] = jax.random.uniform(key, SHAPES[name], jnp.float32, 0.005, 0.015)
    return drawn


def matmul(a, w):
    return jnp.dot(a, w, preferred_element_type=jnp.float32).astype(jnp.bfloat16)


def normed(h):
    wide = h.astype(jnp.float32)
    scale = lax.rsqrt(jnp.mean(wide**2, -1, keepdims=True) + 1e-6)
    return (wide * scale).astype(jnp.bfloat16)


def layer(h, w):
    a = normed(h)
    gate = jnp.dot(a, w["w_gate"], preferred_element_type=jnp.float32)
    up = jnp.dot(a, w["w_up"], preferred_element_type=jnp.float32)
    return h + matmul((jax.nn.silu(gate) * up).astype(jnp.bfloat16), w["w_down"])


def adamw(w, m, v, g):
    m = 0.9 * m + 0.1 * g
    v = 0.95 * v + 0.05 * g * g
    step = m * lax.rsqrt(v + 1e-8) + 0.1 * w
    return (w - 0.02 * step).astype(jnp.bfloat16), m, v


def clipped(gradients, sum_of_squares, count):
    factor = jnp.minimum(1.0, 0.5 * lax.rsqrt(sum_of_squares / count + 1e-30))
    return [g * factor for g in gradients]


def stack(weights, h):
    return lax.scan(lambda h, w: (layer(h, w), None), h, weights)[0]


def reference(x, dy, w_gate, w_up, w_down, m_w_gate, m_w_up, m_w_down, v_w_gate, v_w_up, v_w_down):
    weights = dict(zip(NAMES, (w_gate, w_up, w_down), strict=True))

    def take(so_far, sequence):
        h, by_y = sequence
        _, back = jax.vjp(lambda w: stack(w, h), weights)
        return jax.tree.map(lambda total, term: total + term.astype(jnp.float32), so_far, back(by_y)[0]), None

    none_yet = {name: jnp.zeros(w.shape, jnp.float32) for name, w in weights.items()}
    by_weights, _ = lax.scan(take, none_yet, (x, dy))
    gradients = [by_weights[name].astype(jnp.bfloat16).astype(jnp.float32) for name in NAMES]
    gradients = clipped(gradients, sum(jnp.sum(g * g) for g in gradients), sum(g.size for g in gradients))
    new = [
        adamw(w.astype(jnp.float32), m, v, g)
        for w, m, v, g in zip((w_gate, w_up, w_down), (m_w_gate, m_w_up, m_w_down), (v_w_gate, v_w_up, v_w_down), gradients, strict=True)
    ]
    return tuple(one[which] for which in range(3) for one in new)
```

```python
import functools
import math

import jax
import jax.numpy as jnp
from jax import lax
from jax.experimental import pallas as pl
from jax.experimental.pallas import tpu as pltpu
from jax.sharding import PartitionSpec as P

NAMES = ("w_gate", "w_up", "w_down")
MESH = pl.DeviceIdType.MESH


def matmul(a, w):
    return jnp.dot(a, w, preferred_element_type=jnp.float32).astype(jnp.bfloat16)


def normed(h):
    wide = h.astype(jnp.float32)
    scale = lax.rsqrt(jnp.mean(wide**2, -1, keepdims=True) + 1e-6)
    return (wide * scale).astype(jnp.bfloat16)


def layer(h, w):
    a = normed(h)
    gate = jnp.dot(a, w["w_gate"], preferred_element_type=jnp.float32)
    up = jnp.dot(a, w["w_up"], preferred_element_type=jnp.float32)
    return h + matmul((jax.nn.silu(gate) * up).astype(jnp.bfloat16), w["w_down"])


def factor_kernel(n, count, *refs):
    shards, (out_ref, mine, slots, send_sems, recv_sems) = refs[:-5], refs[-5:]
    me = lax.axis_index("dp")
    barrier = pltpu.get_barrier_semaphore()
    for d in range(1, n):
        pl.semaphore_signal(barrier, inc=1, device_id={"dp": lax.rem(me + d, n)}, device_id_type=MESH)
    total = jnp.zeros((1, 128), jnp.float32)
    for ref in shards:
        g = ref[...].astype(jnp.float32)
        part = jnp.sum(g * g, axis=0, keepdims=True)
        for c in range(0, part.shape[1], 128):
            total = total + part[:, c : c + 128]
    mine[...] = jnp.broadcast_to(total, mine.shape)
    slots[me] = jnp.broadcast_to(total, mine.shape)
    pl.semaphore_wait(barrier, n - 1)
    copies = []
    for d in range(1, n):
        to = lax.rem(me + d, n)
        copy = pltpu.make_async_remote_copy(
            src_ref=mine, dst_ref=slots.at[me], send_sem=send_sems.at[d], recv_sem=recv_sems.at[d], device_id={"dp": to}, device_id_type=MESH
        )
        copy.start()
        copies.append(copy)
    for copy in copies:
        copy.wait_recv()
    for copy in copies:
        copy.wait_send()
    squares = jnp.zeros((8, 128), jnp.float32)
    for i in range(n):
        squares = squares + slots[i]
    squares = jnp.sum(squares[0:1], axis=1, keepdims=True)
    out_ref[...] = jnp.broadcast_to(jnp.minimum(1.0, 0.5 * lax.rsqrt(squares / count + 1e-30)), out_ref.shape)


def clip_factor(shards, n, count):
    return pl.pallas_call(
        functools.partial(factor_kernel, n, count),
        out_shape=jax.ShapeDtypeStruct((8, 128), jnp.float32),
        in_specs=[pl.BlockSpec(memory_space=pltpu.VMEM)] * len(shards),
        out_specs=pl.BlockSpec(memory_space=pltpu.VMEM),
        scratch_shapes=[
            pltpu.VMEM((8, 128), jnp.float32),
            pltpu.VMEM((n, 8, 128), jnp.float32),
            pltpu.SemaphoreType.DMA((n,)),
            pltpu.SemaphoreType.DMA((n,)),
        ],
        compiler_params=pltpu.CompilerParams(collective_id=0, has_side_effects=True, vmem_limit_bytes=16 * 2**20),
        cost_estimate=pl.CostEstimate(flops=10**7, bytes_accessed=2**20, transcendentals=0),
        name="clip_factor",
    )(*shards)


def adamw_kernel(f_ref, g_ref, w_ref, m_ref, v_ref, *rest):
    nw_ref, nm_ref, nv_ref = rest[-3:]
    f = f_ref[0:1, 0:1]
    g = g_ref[...].astype(jnp.float32) * f
    m = 0.9 * m_ref[0] + 0.1 * g
    v = 0.95 * v_ref[0] + 0.05 * g * g
    w = w_ref[0].astype(jnp.float32)
    nm_ref[0] = m
    nv_ref[0] = v
    nw_ref[0] = (w - 0.02 * (m * lax.rsqrt(v + 1e-8) + 0.1 * w)).astype(jnp.bfloat16)


def adamw(number, f, g, w, m, v, before):
    _, rows, cols = w.shape
    block = next(b for b in (128, 112, 96, 64, 32, 16) if rows % b == 0)
    whole = pl.BlockSpec((1, block, cols), lambda i: (number, i, 0))
    outs = [jax.ShapeDtypeStruct(a.shape, a.dtype) for a in (w, m, v)]
    size = rows * cols
    return pl.pallas_call(
        adamw_kernel,
        grid=(rows // block,),
        out_shape=outs,
        in_specs=[pl.BlockSpec((8, 128), lambda i: (0, 0)), pl.BlockSpec((block, cols), lambda i: (i, 0)), whole, whole, whole]
        + [pl.BlockSpec(memory_space=pl.ANY)] * len(before),
        out_specs=[whole] * 3,
        input_output_aliases={5 + i: i for i in range(len(before))},
        compiler_params=pltpu.CompilerParams(vmem_limit_bytes=32 * 2**20),
        cost_estimate=pl.CostEstimate(flops=16 * size * 40, bytes_accessed=22 * size, transcendentals=size),
        name="adamw",
    )(f, g, w, m, v, *before)


def solution(mesh):
    n = mesh.shape["dp"]

    def step(x, dy, *arrays):
        weights, m, v = (arrays[i : i + 3] for i in (0, 3, 6))
        layers = weights[0].shape[0]
        h, kept = x[0], []
        for number in range(layers):
            kept.append(h)
            h = layer(h, {name: w[number] for name, w in zip(NAMES, weights, strict=True)})
        by_h, shards = dy[0], {}
        for number in reversed(range(layers)):
            _, back = jax.vjp(lambda w, h: layer(h, w), {name: w[number] for name, w in zip(NAMES, weights, strict=True)}, kept[number])
            by_w, by_h = back(by_h)
            for i, name in reversed(list(enumerate(NAMES))):
                shards[number, i] = lax.psum_scatter(by_w[name], "dp", scatter_dimension=0, tiled=True)
        f = clip_factor(list(shards.values()), n, float(sum(w.size for w in weights)))
        new = [()] * 3
        for (number, i), shard in shards.items():
            g = lax.all_gather(shard, "dp", axis=0, tiled=True)
            new[i] = adamw(number, f, g, weights[i], m[i], v[i], new[i])
        return tuple(one[which] for which in range(3) for one in new)

    return jax.shard_map(
        step,
        mesh=mesh,
        in_specs=(P(("rep", "dp"), None, None),) * 2 + (P(None, None, None),) * 9,
        out_specs=(P("rep", None, None),) * 9,
        check_vma=False,
    )
```

```python
import functools
import math

import jax
import jax.numpy as jnp
from jax import lax
from jax.experimental import pallas as pl
from jax.experimental.pallas import tpu as pltpu
from jax.sharding import PartitionSpec as P

MESH = pl.DeviceIdType.MESH
BLOCK = 256
LANES = 128
SLOTS = 4
BF16, F32 = jnp.bfloat16, jnp.float32
ANY = pl.BlockSpec(memory_space=pl.ANY)
VMEM = pl.BlockSpec(memory_space=pltpu.VMEM)


def dot(a, b, over=((1,), (0,))):
    return lax.dot_general(a, b, (over, ((), ())), preferred_element_type=F32)


def normed(wide):
    return (wide * lax.rsqrt(jnp.mean(wide * wide, -1, keepdims=True) + 1e-6)).astype(BF16)


def forward_kernel(x_ref, dy_ref, wg_ref, wu_ref, wd_ref, a_ref, at_ref, h_ref, dyt_ref, act):
    x = x_ref[0].astype(F32)
    a = normed(x)
    a_ref[0] = a
    at_ref[0] = a.T
    for b in range(wg_ref.shape[2] // BLOCK):
        cols = slice(b * BLOCK, (b + 1) * BLOCK)
        gate, up = dot(a, wg_ref[0, :, cols]), dot(a, wu_ref[0, :, cols])
        act[:, cols] = (gate * jax.nn.sigmoid(gate) * up).astype(BF16)
    dyt_ref[...] = dy_ref[0].T
    h = (x + dot(act[...], wd_ref[0]).astype(BF16).astype(F32)).astype(BF16)
    h_ref[...] = h
    a = normed(h.astype(F32))
    a_ref[1] = a
    at_ref[1] = a.T


def forward(x, dy, wg, wu, wd):
    _, tokens, d = x.shape
    ff = wg.shape[2]
    rows = min(512, tokens)
    tall = pl.BlockSpec((1, rows, d), lambda i: (0, i, 0))
    out = [((2, tokens, d), (2, rows, d), lambda i: (0, i, 0)), ((2, d, tokens), (2, d, rows), lambda i: (0, 0, i))]
    out += [((tokens, d), (rows, d), lambda i: (i, 0)), ((d, tokens), (d, rows), lambda i: (0, i))]
    return pl.pallas_call(
        forward_kernel,
        grid=(tokens // rows,),
        out_shape=[jax.ShapeDtypeStruct(s, BF16) for s, _, _ in out],
        in_specs=[tall, tall]
        + [pl.BlockSpec((1, *w.shape[1:]), lambda i: (0, 0, 0), pipeline_mode=pl.Buffered(1)) for w in (wg, wu, wd)],
        out_specs=[pl.BlockSpec(b, m) for _, b, m in out],
        scratch_shapes=[pltpu.VMEM((rows, ff), BF16)],
        compiler_params=pltpu.CompilerParams(vmem_limit_bytes=60 * 2**20),
        cost_estimate=pl.CostEstimate(flops=6 * tokens * d * ff, bytes_accessed=2 * (9 * tokens * d + 3 * d * ff), transcendentals=tokens * ff),
        name="forward",
    )(x, dy, wg, wu, wd)


def places(side):
    me = lax.axis_index("dp")
    x, y = me // side, me % side
    along_x = lambda d: lax.rem(x + side + d, side) * side + y
    along_y = lambda d: x * side + lax.rem(y + side + d, side)
    return ((x, y, along_x, along_y), (y, x, along_y, along_x))


def backward_kernel(side, a_hbm, at_hbm, h_hbm, dy_hbm, dyt_hbm, wg_hbm, wu_hbm, wd_hbm, out_ref, sq_ref, *scratch):
    (A, AT, H, DY, DYT, ACT, DG, DU, WB, WD, WG1, WU1, TERM, R1, R2, R3, R4, ACC, SA, SB, load_sems, w_sems, send_sems, recv_sems) = scratch
    tokens, d = A.shape
    ff = DG.shape[1]
    nb = ff // BLOCK
    chunks = 2 * nb
    rows = min(512, tokens)
    pr = d // side**2
    spots = places(side)
    wrap = lambda v: lax.rem(v, side)

    def remote(src, dst, stage, slot, h, way, to):
        return pltpu.make_async_remote_copy(
            src_ref=src, dst_ref=dst, send_sem=send_sems.at[stage, slot, h, way], recv_sem=recv_sems.at[stage, slot, h, way],
            device_id={"dp": to}, device_id_type=MESH,
        )

    def message(stage, slot, h, way):
        p, q, to_p, to_q = spots[h]
        step = 1 - 2 * way
        if stage == 0:
            return remote(TERM.at[slot, h, wrap(p + 2), pl.ds(2 * way, 2)], R1.at[slot, h, way], 0, slot, h, way, to_p(step))
        if stage == 1:
            return remote(TERM.at[slot, h, wrap(p + side + step)], R2.at[slot, h, way], 1, slot, h, way, to_p(step))
        if stage == 2:
            part = pl.ds(2 * way, 2 - way)
            return remote(SA.at[slot, h, part], R3.at[slot, h, part], 2, slot, h, way, to_q(step))
        return remote(SB.at[slot, h, way], R4.at[slot, h, way], 3, slot, h, way, to_q(step))

    def both(stage, slot, h, what):
        for way in range(2):
            getattr(message(stage, slot, h, way), what)()

    def stage0(c):
        for h in range(2):
            both(0, c % SLOTS, h, "start")

    def stage1(c):
        slot = c % SLOTS
        for h in range(2):
            p = spots[h][0]
            both(0, slot, h, "wait_recv")
            both(0, slot, h, "wait_send")
            for way, at in ((0, wrap(p + 1)), (1, wrap(p + side - 1))):
                half = pl.ds(2 * way, 2)
                TERM[slot, h, at, half] = (TERM[slot, h, at, half].astype(F32) + R1[slot, h, way].astype(F32)).astype(BF16)
            both(1, slot, h, "start")

    def stage2(c):
        slot = c % SLOTS
        for h in range(2):
            p, q = spots[h][:2]
            both(1, slot, h, "wait_recv")
            both(1, slot, h, "wait_send")
            for o in range(side):
                ACC[slot, h, o] = TERM[slot, h, p, o].astype(F32) + R2[slot, h, 0, o].astype(F32) + R2[slot, h, 1, o].astype(F32)
            SA[slot, h] = ACC[slot, h, wrap(q + 2)].astype(BF16)
            both(2, slot, h, "start")

    def stage3(c):
        slot = c % SLOTS
        for h in range(2):
            q = spots[h][1]
            both(2, slot, h, "wait_recv")
            both(2, slot, h, "wait_send")
            after, before = wrap(q + 1), wrap(q + side - 1)
            SB[slot, h, 0, 0:2] = (ACC[slot, h, after, 0:2] + R3[slot, h, 0:2].astype(F32)).astype(BF16)
            SB[slot, h, 0, 2:3] = ACC[slot, h, after, 2:3].astype(BF16)
            SB[slot, h, 1, 0:2] = ACC[slot, h, before, 0:2].astype(BF16)
            SB[slot, h, 1, 2:3] = (ACC[slot, h, before, 2:3] + R3[slot, h, 2:3].astype(F32)).astype(BF16)
            both(3, slot, h, "start")

    def stage4(c):
        slot = c % SLOTS
        for h in range(2):
            q = spots[h][1]
            both(3, slot, h, "wait_recv")
            both(3, slot, h, "wait_send")
            g = (ACC[slot, h, q] + R4[slot, h, 0].astype(F32) + R4[slot, h, 1].astype(F32)).astype(BF16)
            out_ref[h, c] = g
            g = g.astype(F32)
            sq_ref[...] += g[0] * g[0] + g[1] * g[1] + g[2] * g[2]

    def load(which, l=1):
        src, dst = {"A": (a_hbm.at[l], A), "AT": (at_hbm.at[l], AT), "H": (h_hbm, H), "DY": (dy_hbm.at[0], DY), "DYT": (dyt_hbm, DYT),
                    "WG1": (wg_hbm.at[1], WG1), "WU1": (wu_hbm.at[1], WU1)}[which]
        return pltpu.make_async_copy(src, dst, load_sems.at[("A", "AT", "H", "DY", "DYT", "WG1", "WU1").index(which)])

    def weights(i, what):
        l, at, slot = 1 - i // nb, pl.multiple_of((i % nb) * BLOCK, BLOCK), i % 2
        for j, (src, dst) in enumerate((
            (wg_hbm.at[l, :, pl.ds(at, BLOCK)], WB.at[slot, 0]),
            (wu_hbm.at[l, :, pl.ds(at, BLOCK)], WB.at[slot, 1]),
            (wd_hbm.at[l, pl.ds(at, BLOCK), :], WD.at[slot]),
        )):
            getattr(pltpu.make_async_copy(src, dst, w_sems.at[slot, j]), what)()

    def middle():
        load("A", 0).start()
        load("AT", 0).start()
        for which in ("H", "WG1", "WU1"):
            load(which).wait()
        for t in range(tokens // rows):
            at = slice(t * rows, (t + 1) * rows)
            by_a = dot(DG[at, :], WG1[...], ((1,), (1,))).astype(BF16).astype(F32)
            by_a = (by_a + dot(DU[at, :], WU1[...], ((1,), (1,))).astype(BF16).astype(F32)).astype(BF16).astype(F32)
            wide = H[at, :].astype(F32)
            scale = lax.rsqrt(jnp.mean(wide * wide, -1, keepdims=True) + 1e-6)
            by_scale = jnp.sum(by_a * wide, -1, keepdims=True)
            by_wide = (by_a * scale - wide * (by_scale * scale * scale * scale * (1.0 / d))).astype(BF16).astype(F32)
            by_h = (DY[at, :].astype(F32) + by_wide).astype(BF16)
            DY[at, :] = by_h
            DYT[:, at] = by_h.T
        load("A", 0).wait()
        load("AT", 0).wait()

    def compute(i):
        slot, ws = i % SLOTS, i % 2
        cols = pl.ds(pl.multiple_of((i % nb) * BLOCK, BLOCK), BLOCK)
        weights(i, "wait")

        @pl.when(i + 1 < chunks)
        def _():
            weights(i + 1, "start")

        for t in range(tokens // rows):
            at = slice(t * rows, (t + 1) * rows)
            gate, up = dot(A[at, :], WB[ws, 0]), dot(A[at, :], WB[ws, 1])
            by_act = dot(DY[at, :], WD[ws], ((1,), (1,))).astype(BF16).astype(F32)
            sig = jax.nn.sigmoid(gate)
            silu = gate * sig
            ACT[at, :] = (silu * up).astype(BF16)
            DU[at, cols] = (by_act * silu).astype(BF16)
            DG[at, cols] = (by_act * up * (sig * (1.0 + gate * (1.0 - sig)))).astype(BF16)

        @pl.when(i == 0)
        def _():
            load("AT").wait()
            load("DYT").wait()

        for j, (left, right) in enumerate(((AT, DG[:, cols]), (AT, DU[:, cols]), (DYT, ACT[...]))):
            g = dot(left[...], right).astype(BF16)
            for o in range(side):
                piece = g[o * side * pr : (o + 1) * side * pr].reshape(side, pr, BLOCK)
                for h in range(2):
                    TERM[slot, h, o, :, j] = piece[:, :, h * LANES : (h + 1) * LANES]

    for which in ("A", "DY", "AT", "DYT", "H", "WG1", "WU1"):
        load(which).start()
    weights(0, "start")
    barrier = pltpu.get_barrier_semaphore()
    for h in range(2):
        for step in (1, -1):
            pl.semaphore_signal(barrier, inc=1, device_id={"dp": spots[h][2](step)}, device_id_type=MESH)
    sq_ref[...] = jnp.zeros_like(sq_ref)
    load("A").wait()
    load("DY").wait()
    pl.semaphore_wait(barrier, 4)

    @pl.loop(0, chunks + 4)
    def _(i):
        pl.when(i == nb)(middle)
        pl.when(i < chunks)(lambda: compute(i))
        pl.when(i < chunks)(lambda: stage0(i))
        for lag, stage in enumerate((stage1, stage2, stage3, stage4), 1):
            pl.when((i >= lag) & (i < chunks + lag))(functools.partial(stage, i - lag))


def backward(side, a, at, h, dy, dyt, wg, wu, wd):
    _, tokens, d = a.shape
    ff = wg.shape[2]
    chunks = 2 * (ff // BLOCK)
    pr = d // side**2
    piece = (3, pr, LANES)
    v = pltpu.VMEM
    sems = pltpu.SemaphoreType.DMA
    return pl.pallas_call(
        functools.partial(backward_kernel, side),
        out_shape=[jax.ShapeDtypeStruct((2, chunks, *piece), BF16), jax.ShapeDtypeStruct((pr, LANES), F32)],
        in_specs=[ANY] * 8,
        out_specs=[VMEM] * 2,
        scratch_shapes=[
            v((tokens, d), BF16), v((d, tokens), BF16), v((tokens, d), BF16), v((tokens, d), BF16), v((d, tokens), BF16),
            v((tokens, BLOCK), BF16), v((tokens, ff), BF16), v((tokens, ff), BF16),
            v((2, 2, d, BLOCK), BF16), v((2, BLOCK, d), BF16), v((d, ff), BF16), v((d, ff), BF16),
            v((SLOTS, 2, side, side, *piece), BF16), v((SLOTS, 2, 2, 2, *piece), BF16), v((SLOTS, 2, 2, side, *piece), BF16),
            v((SLOTS, 2, *piece), BF16), v((SLOTS, 2, 2, *piece), BF16), v((SLOTS, 2, side, *piece), F32),
            v((SLOTS, 2, *piece), BF16), v((SLOTS, 2, 2, *piece), BF16),
            sems((7,)), sems((2, 3)), sems((4, SLOTS, 2, 2)), sems((4, SLOTS, 2, 2)),
        ],
        compiler_params=pltpu.CompilerParams(collective_id=0, has_side_effects=True, vmem_limit_bytes=67043328),
        cost_estimate=pl.CostEstimate(flops=28 * tokens * d * ff, bytes_accessed=2 * (7 * tokens * d + 8 * d * ff), transcendentals=2 * tokens * ff),
        name="backward",
    )(a, at, h, dy, dyt, wg, wu, wd)


def gather_kernel(side, count, groups, shard_ref, sq_ref, g_ref, f_ref, mine, slots, sq_sems, send_sems, recv_sems, own_sems):
    n = side * side
    me = lax.axis_index("dp")
    spots = places(side)
    wrap = lambda v: lax.rem(v + side, side)
    barrier = pltpu.get_barrier_semaphore()
    for d in range(1, n):
        pl.semaphore_signal(barrier, inc=1, device_id={"dp": lax.rem(me + d, n)}, device_id_type=MESH)
    squares = jnp.broadcast_to(jnp.sum(sq_ref[...], axis=0, keepdims=True), mine.shape)
    mine[...] = squares
    slots[me] = squares
    own = []
    for h, (p, q, _, _) in enumerate(spots):
        own.append(pltpu.make_async_copy(shard_ref.at[h], g_ref.at[h, p, q], own_sems.at[h]))
        own[-1].start()
    pl.semaphore_wait(barrier, n - 1)
    sent = []
    for d in range(1, n):
        copy = pltpu.make_async_remote_copy(
            src_ref=mine, dst_ref=slots.at[me], send_sem=sq_sems.at[0, d], recv_sem=sq_sems.at[1, d],
            device_id={"dp": lax.rem(me + d, n)}, device_id_type=MESH,
        )
        copy.start()
        sent.append(copy)
    factors = list(sent)

    def piece(k, h, dp, dq):
        p, q = spots[h][:2]
        return g_ref.at[h, wrap(p - dp), wrap(q - dq), pl.ds(*groups[k])]

    def send(k, h, dp, dq, to, own=False, come=None):
        src = shard_ref.at[h, pl.ds(*groups[k])] if own else piece(k, h, dp, dq)
        index = come[0] * side + come[1]
        copy = pltpu.make_async_remote_copy(
            src_ref=src, dst_ref=piece(k, h, dp, dq), send_sem=send_sems.at[k, h, len(sends[k, h])], recv_sem=recv_sems.at[k, h, index],
            device_id={"dp": to}, device_id_type=MESH,
        )
        copy.start()
        sends[k, h].append(copy)

    def arrived(k, h, dp, dq):
        ref = piece(k, h, dp, dq)
        pltpu.make_async_remote_copy(
            src_ref=ref, dst_ref=ref, send_sem=send_sems.at[k, h, 0], recv_sem=recv_sems.at[k, h, dp * side + dq],
            device_id={"dp": me}, device_id_type=MESH,
        ).wait_recv()

    sends = {(k, h): [] for k in range(len(groups)) for h in range(2)}
    last = side - 1

    def across(k, h, dq, own=False):
        to_p = spots[h][2]
        send(k, h, 0, dq, to_p(1), own, (1, dq))
        send(k, h, 0, dq, to_p(-1), own, (last, dq))

    def begin(k):
        for h in range(2):
            to_q = spots[h][3]
            send(k, h, 0, 0, to_q(1), True, (0, 1))
            send(k, h, 0, 0, to_q(-1), True, (0, last))
        for h in range(2):
            across(k, h, 0, True)

    def first(k):
        for h in range(2):
            to_q = spots[h][3]
            arrived(k, h, 0, 1)
            arrived(k, h, 0, last)
            if (k + h) % 2:
                send(k, h, 0, last, to_q(-1), come=(0, 2))
            else:
                send(k, h, 0, 1, to_q(1), come=(0, 2))
            across(k, h, 1)
            across(k, h, last)

    def second(k):
        for h in range(2):
            arrived(k, h, 0, 2)
            across(k, h, 2)

    def third(k):
        for h in range(2):
            to_p = spots[h][2]
            for dq in (0, 1, last, 2):
                arrived(k, h, 1, dq)
                arrived(k, h, last, dq)
                if dq % 2:
                    send(k, h, last, dq, to_p(-1), come=(2, dq))
                else:
                    send(k, h, 1, dq, to_p(1), come=(2, dq))

    def fourth(k):
        for h in range(2):
            for dq in range(side):
                arrived(k, h, 2, dq)

    for s in range(len(groups) + 3):
        for lag, stages in enumerate(((begin,), (first, second), (third,), (fourth,))):
            if 0 <= s - lag < len(groups):
                for stage in stages:
                    stage(s - lag)
        if s == 1:
            for copy in factors:
                copy.wait_recv()
            total = jnp.zeros((8, LANES), F32)
            for i in range(n):
                total = total + slots[i]
            total = jnp.sum(total[0:1], axis=1, keepdims=True)
            f_ref[...] = jnp.broadcast_to(jnp.minimum(1.0, 0.5 * lax.rsqrt(total / count + 1e-30)), f_ref.shape)
    for copies in sends.values():
        sent.extend(copies)
    for copy in sent:
        copy.wait_send()
    for copy in own:
        copy.wait()


def gather(side, count, shard, sq):
    chunks = shard.shape[1]
    size = max(1, chunks // 4 + (chunks % 4 > 0))
    groups = [(c, min(size, chunks - c)) for c in range(0, chunks, size)]
    n = side * side
    sems = pltpu.SemaphoreType.DMA
    return pl.pallas_call(
        functools.partial(gather_kernel, side, count, groups),
        out_shape=[jax.ShapeDtypeStruct((2, side, side, *shard.shape[1:]), BF16), jax.ShapeDtypeStruct((8, LANES), F32)],
        in_specs=[VMEM, VMEM],
        out_specs=[ANY, VMEM],
        scratch_shapes=[
            pltpu.VMEM((8, LANES), F32), pltpu.VMEM((n, 8, LANES), F32), sems((2, n)),
            sems((len(groups), 2, n - 1)), sems((len(groups), 2, n)), sems((2,)),
        ],
        compiler_params=pltpu.CompilerParams(collective_id=1, has_side_effects=True, vmem_limit_bytes=60 * 2**20),
        cost_estimate=pl.CostEstimate(flops=10**8, bytes_accessed=2 * n * shard.size, transcendentals=0),
        name="gather",
    )(shard, sq)


def adamw(f, g, w, m, v):
    g = g.astype(F32) * f
    m = 0.9 * m + 0.1 * g
    v = 0.95 * v + 0.05 * g * g
    w = w.astype(F32)
    return (w - 0.02 * (m * lax.rsqrt(v + 1e-8) + 0.1 * w)).astype(BF16), m, v


def wide_kernel(f_ref, g_ref, *refs):
    f = f_ref[0:1, 0:1]
    for j in range(2):
        w, m, v, nw, nm, nv = refs[j::2]
        _, _, places_, nb, _, pr, _ = g_ref.shape
        for b in range(nb):
            for h in range(2):
                cols = slice((2 * b + h) * LANES, (2 * b + h + 1) * LANES)
                g = g_ref[h, 0, :, b, j].reshape(places_ * pr, LANES)
                nw[0, :, cols], nm[0, :, cols], nv[0, :, cols] = adamw(f, g, w[0, :, cols], m[0, :, cols], v[0, :, cols])


def tall_kernel(f_ref, g_ref, w, m, v, nw, nm, nv):
    f = f_ref[0:1, 0:1]
    _, side, _, _, _, pr, _ = g_ref.shape
    for h in range(2):
        rows = slice(h * LANES, (h + 1) * LANES)
        g = g_ref[h, :, :, 0, 0].reshape(side * side * pr, LANES).T
        nw[0, rows, :], nm[0, rows, :], nv[0, rows, :] = adamw(f, g, w[0, rows, :], m[0, rows, :], v[0, rows, :])


def update_wide(f, g, weights, m, v):
    arrays = (*weights, *m, *v)
    layers, d, ff = weights[0].shape
    _, side, _, chunks, _, pr, _ = g.shape
    nb = chunks // layers
    block = pl.BlockSpec((1, d // side, ff), lambda l, i: (l, i, 0))
    return pl.pallas_call(
        wide_kernel,
        grid=(layers, side),
        out_shape=[jax.ShapeDtypeStruct(a.shape, a.dtype) for a in arrays],
        in_specs=[pl.BlockSpec((8, LANES), lambda l, i: (0, 0)),
                  pl.BlockSpec((2, 1, side, nb, 2, pr, LANES), lambda l, i: (0, i, 0, layers - 1 - l, 0, 0, 0))] + [block] * 6,
        out_specs=[block] * 6,
        compiler_params=pltpu.CompilerParams(vmem_limit_bytes=60 * 2**20),
        cost_estimate=pl.CostEstimate(flops=30 * layers * d * ff, bytes_accessed=44 * layers * d * ff, transcendentals=2 * layers * d * ff),
        name="update_wide",
    )(f, g, *arrays)


def update_tall(f, g, w, m, v):
    layers, ff, d = w.shape
    _, side, _, chunks, _, pr, _ = g.shape
    nb = chunks // layers
    block = pl.BlockSpec((1, BLOCK, d), lambda l, b: (l, b, 0))
    return pl.pallas_call(
        tall_kernel,
        grid=(layers, nb),
        out_shape=[jax.ShapeDtypeStruct(a.shape, a.dtype) for a in (w, m, v)],
        in_specs=[pl.BlockSpec((8, LANES), lambda l, b: (0, 0)),
                  pl.BlockSpec((2, side, side, 1, 1, pr, LANES), lambda l, b: (0, 0, 0, (layers - 1 - l) * nb + b, 2, 0, 0))] + [block] * 3,
        out_specs=[block] * 3,
        compiler_params=pltpu.CompilerParams(vmem_limit_bytes=60 * 2**20),
        cost_estimate=pl.CostEstimate(flops=15 * layers * d * ff, bytes_accessed=22 * layers * d * ff, transcendentals=layers * d * ff),
        name="update_tall",
    )(f, g, w, m, v)


def solution(mesh):
    side = math.isqrt(mesh.shape["dp"])

    def step(x, dy, wg, wu, wd, mg, mu, md, vg, vu, vd):
        a, at, h, dyt = forward(x, dy, wg, wu, wd)
        shard, sq = backward(side, a, at, h, dy, dyt, wg, wu, wd)
        g, f = gather(side, float(wg.size + wu.size + wd.size), shard, sq)
        new = update_wide(f, g, (wg, wu), (mg, mu), (vg, vu))
        nwd, nmd, nvd = update_tall(f, g, wd, md, vd)
        return new[0], new[1], nwd, new[2], new[3], nmd, new[4], new[5], nvd

    return jax.shard_map(
        step,
        mesh=mesh,
        in_specs=(P(("rep", "dp"), None, None),) * 2 + (P(None, None, None),) * 9,
        out_specs=(P("rep", None, None),) * 9,
        check_vma=False,
    )
```

```python
import functools
import math

import jax
import jax.numpy as jnp
from jax import lax
from jax.experimental import pallas as pl
from jax.experimental.pallas import tpu as pltpu
from jax.sharding import PartitionSpec as P

MESH = pl.DeviceIdType.MESH
BLOCK = 256
LANES = 128
SLOTS = 4
BF16, F32 = jnp.bfloat16, jnp.float32
ANY = pl.BlockSpec(memory_space=pl.ANY)
VMEM = pl.BlockSpec(memory_space=pltpu.VMEM)


def dot(a, b, over=((1,), (0,))):
    return lax.dot_general(a, b, (over, ((), ())), preferred_element_type=F32)


def normed(wide):
    return (wide * lax.rsqrt(jnp.mean(wide * wide, -1, keepdims=True) + 1e-6)).astype(BF16)


def forward_kernel(x_ref, dy_ref, wg_ref, wu_ref, wd_ref, a_ref, at_ref, h_ref, dyt_ref, act):
    x = x_ref[0].astype(F32)
    a = normed(x)
    a_ref[0] = a
    at_ref[0] = a.T
    for b in range(wg_ref.shape[2] // BLOCK):
        cols = slice(b * BLOCK, (b + 1) * BLOCK)
        gate, up = dot(a, wg_ref[0, :, cols]), dot(a, wu_ref[0, :, cols])
        act[:, cols] = (gate * jax.nn.sigmoid(gate) * up).astype(BF16)
    dyt_ref[...] = dy_ref[0].T
    h = (x + dot(act[...], wd_ref[0]).astype(BF16).astype(F32)).astype(BF16)
    h_ref[...] = h
    a = normed(h.astype(F32))
    a_ref[1] = a
    at_ref[1] = a.T


def forward(x, dy, wg, wu, wd):
    _, tokens, d = x.shape
    ff = wg.shape[2]
    rows = min(512, tokens)
    tall = pl.BlockSpec((1, rows, d), lambda i: (0, i, 0))
    out = [((2, tokens, d), (2, rows, d), lambda i: (0, i, 0)), ((2, d, tokens), (2, d, rows), lambda i: (0, 0, i))]
    out += [((tokens, d), (rows, d), lambda i: (i, 0)), ((d, tokens), (d, rows), lambda i: (0, i))]
    return pl.pallas_call(
        forward_kernel,
        grid=(tokens // rows,),
        out_shape=[jax.ShapeDtypeStruct(s, BF16) for s, _, _ in out],
        in_specs=[tall, tall]
        + [pl.BlockSpec((1, *w.shape[1:]), lambda i: (0, 0, 0), pipeline_mode=pl.Buffered(1)) for w in (wg, wu, wd)],
        out_specs=[pl.BlockSpec(b, m) for _, b, m in out],
        scratch_shapes=[pltpu.VMEM((rows, ff), BF16)],
        compiler_params=pltpu.CompilerParams(vmem_limit_bytes=60 * 2**20),
        cost_estimate=pl.CostEstimate(flops=6 * tokens * d * ff, bytes_accessed=2 * (9 * tokens * d + 3 * d * ff), transcendentals=tokens * ff),
        name="forward",
    )(x, dy, wg, wu, wd)


def places(side):
    me = lax.axis_index("dp")
    x, y = me // side, me % side
    along_x = lambda d: lax.rem(x + side + d, side) * side + y
    along_y = lambda d: x * side + lax.rem(y + side + d, side)
    return ((x, y, along_x, along_y), (y, x, along_y, along_x))


def backward_kernel(side, count, a_hbm, at_hbm, h_hbm, dy_hbm, dyt_hbm, wg_hbm, wu_hbm, wd_hbm, *refs):
    set_d, set_gu, f_ref, scratch = refs[0:2], (refs[2:4], refs[4:6]), refs[6], refs[7:]
    (A, AT, H, DY, DYT, ACT, DG, DU, WB, WD, WG1, WU1, TERM, R1, R2, R3, R4, ACC, SA, SB, OWN, SQ, MINE, SQS) = scratch[:-6]
    load_sems, w_sems, send_sems, recv_sems, own_sems, sq_sems = scratch[-6:]
    tokens, d = A.shape
    ff = DG.shape[1]
    nb = ff // BLOCK
    chunks = 2 * nb
    rows = min(512, tokens)
    n = side * side
    me = lax.axis_index("dp")
    pr = d // (2 * n)
    spots = places(side)
    wrap = lambda v: lax.rem(v, side)

    def remote(src, dst, stage, slot, h, way, to):
        return pltpu.make_async_remote_copy(
            src_ref=src, dst_ref=dst, send_sem=send_sems.at[stage, slot, h, way], recv_sem=recv_sems.at[stage, slot, h, way],
            device_id={"dp": to}, device_id_type=MESH,
        )

    def message(stage, slot, h, way):
        p, q, to_p, to_q = spots[h]
        step = 1 - 2 * way
        if stage == 0:
            return remote(TERM.at[slot, h, wrap(p + 2), pl.ds(2 * way, 2)], R1.at[slot, h, way], 0, slot, h, way, to_p(step))
        if stage == 1:
            return remote(TERM.at[slot, h, wrap(p + side + step)], R2.at[slot, h, way], 1, slot, h, way, to_p(step))
        if stage == 2:
            part = pl.ds(2 * way, 2 - way)
            return remote(SA.at[slot, h, part], R3.at[slot, h, part], 2, slot, h, way, to_q(step))
        return remote(SB.at[slot, h, way], R4.at[slot, h, way], 3, slot, h, way, to_q(step))

    def both(stage, slot, h, what):
        for way in range(2):
            getattr(message(stage, slot, h, way), what)()

    def stage0(c):
        for h in range(2):
            both(0, c % SLOTS, h, "start")

    def stage1(c):
        slot = c % SLOTS
        for h in range(2):
            p = spots[h][0]
            both(0, slot, h, "wait_recv")
            both(0, slot, h, "wait_send")
            for way, at in ((0, wrap(p + 1)), (1, wrap(p + side - 1))):
                half = pl.ds(2 * way, 2)
                TERM[slot, h, at, half] = (TERM[slot, h, at, half].astype(F32) + R1[slot, h, way].astype(F32)).astype(BF16)
            both(1, slot, h, "start")

    def stage2(c):
        slot = c % SLOTS
        for h in range(2):
            p, q = spots[h][:2]
            both(1, slot, h, "wait_recv")
            both(1, slot, h, "wait_send")
            for o in range(side):
                ACC[slot, h, o] = TERM[slot, h, p, o].astype(F32) + R2[slot, h, 0, o].astype(F32) + R2[slot, h, 1, o].astype(F32)
            SA[slot, h] = ACC[slot, h, wrap(q + 2)].astype(BF16)
            both(2, slot, h, "start")

    def stage3(c):
        slot = c % SLOTS
        for h in range(2):
            q = spots[h][1]
            both(2, slot, h, "wait_recv")
            both(2, slot, h, "wait_send")
            after, before = wrap(q + 1), wrap(q + side - 1)
            SB[slot, h, 0, 0:2] = (ACC[slot, h, after, 0:2] + R3[slot, h, 0:2].astype(F32)).astype(BF16)
            SB[slot, h, 0, 2:3] = ACC[slot, h, after, 2:3].astype(BF16)
            SB[slot, h, 1, 0:2] = ACC[slot, h, before, 0:2].astype(BF16)
            SB[slot, h, 1, 2:3] = (ACC[slot, h, before, 2:3] + R3[slot, h, 2:3].astype(F32)).astype(BF16)
            both(3, slot, h, "start")

    def by_layer(c, do):
        for l in range(2):
            pl.when(c // nb == 1 - l)(functools.partial(do, l))

    def gather_message(part, l, slot, h, way, c):
        q, to_q = spots[h][1], spots[h][3]
        step = 1 - 2 * way
        at = q if part < 2 else wrap(q + side - step)
        dst = set_gu[l][h].at[at, c % nb] if part % 2 == 0 else set_d[h].at[at, c]
        src = (OWN.at[slot, h, pl.ds(0, 2)] if part == 0 else OWN.at[slot, h, 2]) if part < 2 else dst
        return remote(src, dst, 4 + part, slot, h, way, to_q(step))

    def own_copy(part, l, slot, h, c):
        q = spots[h][1]
        if part == 0:
            return pltpu.make_async_copy(OWN.at[slot, h, pl.ds(0, 2)], set_gu[l][h].at[q, c % nb], own_sems.at[slot, h, 0])
        return pltpu.make_async_copy(OWN.at[slot, h, 2], set_d[h].at[q, c], own_sems.at[slot, h, 1])

    def stage4(c):
        slot = c % SLOTS
        for h in range(2):
            q = spots[h][1]
            both(3, slot, h, "wait_recv")
            both(3, slot, h, "wait_send")
            g = (ACC[slot, h, q] + R4[slot, h, 0].astype(F32) + R4[slot, h, 1].astype(F32)).astype(BF16)
            OWN[slot, h] = g
            g = g.astype(F32)
            SQ[...] += g[0] * g[0] + g[1] * g[1] + g[2] * g[2]

            def gate_up(l, h=h):
                own_copy(0, l, slot, h, c).start()
                for way in range(2):
                    gather_message(0, l, slot, h, way, c).start()

            by_layer(c, gate_up)
            own_copy(1, 0, slot, h, c).start()
            for way in range(2):
                gather_message(1, 0, slot, h, way, c).start()

    def stage5(c):
        slot = c % SLOTS
        for h in range(2):
            for part in range(2):
                for way in range(2):
                    copy = gather_message(part, 0, slot, h, way, c)
                    copy.wait_recv()
                    copy.wait_send()
                own_copy(part, 0, slot, h, c).wait()
            by_layer(c, lambda l, h=h: gather_message(2, l, slot, h, 0, c).start())
            gather_message(3, 0, slot, h, 1, c).start()

    def stage6(c):
        slot = c % SLOTS
        for h in range(2):
            for part, way in ((2, 0), (3, 1)):
                copy = gather_message(part, 0, slot, h, way, c)
                copy.wait_recv()
                copy.wait_send()

    def square(d):
        return pltpu.make_async_remote_copy(
            src_ref=MINE, dst_ref=SQS.at[me], send_sem=sq_sems.at[0, d], recv_sem=sq_sems.at[1, d],
            device_id={"dp": lax.rem(me + d, n)}, device_id_type=MESH,
        )

    def squares():
        total = jnp.broadcast_to(jnp.sum(SQ[...], axis=0, keepdims=True), MINE.shape)
        MINE[...] = total
        SQS[me] = total
        for d in range(1, n):
            square(d).start()

    def load(which, l=1):
        src, dst = {"A": (a_hbm.at[l], A), "AT": (at_hbm.at[l], AT), "H": (h_hbm, H), "DY": (dy_hbm.at[0], DY), "DYT": (dyt_hbm, DYT),
                    "WG1": (wg_hbm.at[1], WG1), "WU1": (wu_hbm.at[1], WU1)}[which]
        return pltpu.make_async_copy(src, dst, load_sems.at[("A", "AT", "H", "DY", "DYT", "WG1", "WU1").index(which)])

    def weights(i, what):
        l, at, slot = 1 - i // nb, pl.multiple_of((i % nb) * BLOCK, BLOCK), i % 2
        for j, (src, dst) in enumerate((
            (wg_hbm.at[l, :, pl.ds(at, BLOCK)], WB.at[slot, 0]),
            (wu_hbm.at[l, :, pl.ds(at, BLOCK)], WB.at[slot, 1]),
            (wd_hbm.at[l, pl.ds(at, BLOCK), :], WD.at[slot]),
        )):
            getattr(pltpu.make_async_copy(src, dst, w_sems.at[slot, j]), what)()

    def middle():
        load("A", 0).start()
        load("AT", 0).start()
        for which in ("H", "WG1", "WU1"):
            load(which).wait()
        for t in range(tokens // rows):
            at = slice(t * rows, (t + 1) * rows)
            by_a = dot(DG[at, :], WG1[...], ((1,), (1,))).astype(BF16).astype(F32)
            by_a = (by_a + dot(DU[at, :], WU1[...], ((1,), (1,))).astype(BF16).astype(F32)).astype(BF16).astype(F32)
            wide = H[at, :].astype(F32)
            scale = lax.rsqrt(jnp.mean(wide * wide, -1, keepdims=True) + 1e-6)
            by_scale = jnp.sum(by_a * wide, -1, keepdims=True)
            by_wide = (by_a * scale - wide * (by_scale * scale * scale * scale * (1.0 / d))).astype(BF16).astype(F32)
            by_h = (DY[at, :].astype(F32) + by_wide).astype(BF16)
            DY[at, :] = by_h
            DYT[:, at] = by_h.T
        load("A", 0).wait()
        load("AT", 0).wait()

    def compute(i):
        slot, ws = i % SLOTS, i % 2
        cols = pl.ds(pl.multiple_of((i % nb) * BLOCK, BLOCK), BLOCK)
        weights(i, "wait")

        @pl.when(i + 1 < chunks)
        def _():
            weights(i + 1, "start")

        for t in range(tokens // rows):
            at = slice(t * rows, (t + 1) * rows)
            gate, up = dot(A[at, :], WB[ws, 0]), dot(A[at, :], WB[ws, 1])
            by_act = dot(DY[at, :], WD[ws], ((1,), (1,))).astype(BF16).astype(F32)
            sig = jax.nn.sigmoid(gate)
            silu = gate * sig
            ACT[at, :] = (silu * up).astype(BF16)
            DU[at, cols] = (by_act * silu).astype(BF16)
            DG[at, cols] = (by_act * up * (sig * (1.0 + gate * (1.0 - sig)))).astype(BF16)

        @pl.when(i == 0)
        def _():
            load("AT").wait()
            load("DYT").wait()

        for j, (left, right) in enumerate(((AT, DG[:, cols]), (AT, DU[:, cols]), (DYT, ACT[...]))):
            g = dot(left[...], right)
            for o in range(2 * side):
                piece = g[o * side * pr : (o + 1) * side * pr].reshape(side, pr, BLOCK)
                TERM[slot, o // side, o % side, :, j] = piece.astype(BF16)

    for which in ("A", "DY", "AT", "DYT", "H", "WG1", "WU1"):
        load(which).start()
    weights(0, "start")
    barrier = pltpu.get_barrier_semaphore()
    for other in range(1, n):
        pl.semaphore_signal(barrier, inc=1, device_id={"dp": lax.rem(me + other, n)}, device_id_type=MESH)
    SQ[...] = jnp.zeros_like(SQ)
    load("A").wait()
    load("DY").wait()
    pl.semaphore_wait(barrier, n - 1)

    @pl.loop(0, chunks + 6)
    def _(i):
        pl.when(i == nb)(middle)
        pl.when(i < chunks)(lambda: compute(i))
        pl.when(i < chunks)(lambda: stage0(i))
        for lag, stage in enumerate((stage1, stage2, stage3, stage4, stage5, stage6), 1):
            pl.when((i >= lag) & (i < chunks + lag))(functools.partial(stage, i - lag))
        pl.when(i == chunks + 3)(squares)

    for other in range(1, n):
        square(other).wait_recv()
    for other in range(1, n):
        square(other).wait_send()
    total = jnp.zeros(MINE.shape, F32)
    for device in range(n):
        total = total + SQS[device]
    total = jnp.sum(total[0:1], axis=1, keepdims=True)
    f_ref[...] = jnp.broadcast_to(jnp.minimum(1.0, 0.5 * lax.rsqrt(total / count + 1e-30)), f_ref.shape)


def backward(side, count, a, at, h, dy, dyt, wg, wu, wd):
    _, tokens, d = a.shape
    ff = wg.shape[2]
    nb = ff // BLOCK
    pr = d // (2 * side**2)
    piece = (3, pr, BLOCK)
    v = pltpu.VMEM
    sems = pltpu.SemaphoreType.DMA
    shapes = [(side, 2 * nb, pr, BLOCK)] * 2 + [(side, nb, 2, pr, BLOCK)] * 4
    out = pl.pallas_call(
        functools.partial(backward_kernel, side, count),
        out_shape=[jax.ShapeDtypeStruct(s, BF16) for s in shapes] + [jax.ShapeDtypeStruct((8, LANES), F32)],
        in_specs=[ANY] * 8,
        out_specs=[ANY] * 6 + [VMEM],
        scratch_shapes=[
            v((tokens, d), BF16), v((d, tokens), BF16), v((tokens, d), BF16), v((tokens, d), BF16), v((d, tokens), BF16),
            v((tokens, BLOCK), BF16), v((tokens, ff), BF16), v((tokens, ff), BF16),
            v((2, 2, d, BLOCK), BF16), v((2, BLOCK, d), BF16), v((d, ff), BF16), v((d, ff), BF16),
            v((SLOTS, 2, side, side, *piece), BF16), v((SLOTS, 2, 2, 2, *piece), BF16), v((SLOTS, 2, 2, side, *piece), BF16),
            v((SLOTS, 2, *piece), BF16), v((SLOTS, 2, 2, *piece), BF16), v((SLOTS, 2, side, *piece), F32),
            v((SLOTS, 2, *piece), BF16), v((SLOTS, 2, 2, *piece), BF16), v((SLOTS, 2, *piece), BF16),
            v((pr, BLOCK), F32), v((8, BLOCK), F32), v((side**2, 8, BLOCK), F32),
            sems((7,)), sems((2, 3)), sems((8, SLOTS, 2, 2)), sems((8, SLOTS, 2, 2)), sems((SLOTS, 2, 2)), sems((2, side**2)),
        ],
        compiler_params=pltpu.CompilerParams(collective_id=0, has_side_effects=True, vmem_limit_bytes=67043328),
        cost_estimate=pl.CostEstimate(flops=28 * tokens * d * ff, bytes_accessed=2 * (7 * tokens * d + 8 * d * ff), transcendentals=2 * tokens * ff),
        name="backward",
    )(a, at, h, dy, dyt, wg, wu, wd)
    return out[0:2], (out[2:4], out[4:6]), out[6]


def adamw(f, g, w, m, v):
    g = g.astype(F32) * f
    m = 0.9 * m + 0.1 * g
    v = 0.95 * v + 0.05 * g * g
    w = w.astype(F32)
    return (w - 0.02 * (m * lax.rsqrt(v + 1e-8) + 0.1 * w)).astype(BF16), m, v


def wide_kernel(starts, layer_of, row_of, f_ref, *refs):
    count = len(starts) - 1
    parts, ins, outs = refs[:count], refs[count : count + 6], refs[-6:]
    f = f_ref[0:1, 0:1]
    step = pl.program_id(0)
    for s in range(count):

        @pl.when((step >= starts[s]) & (step < starts[s + 1]))
        def _(part=parts[s]):
            for j in range(2):
                w, m, v = ins[j::2]
                nw, nm, nv = outs[j::2]
                for b in range(part.shape[1]):
                    cols = slice(b * BLOCK, (b + 1) * BLOCK)
                    nw[0, :, cols], nm[0, :, cols], nv[0, :, cols] = adamw(f, part[0, b, j], w[0, :, cols], m[0, :, cols], v[0, :, cols])


def update_wide(f, parts, arrays, before):
    _, _, ff = arrays[0].shape
    rows = parts[0][0].shape[3]
    starts, layers, blocks = [0], [], []
    for g, l, first in parts:
        starts.append(starts[-1] + g.shape[0])
        layers += [l] * g.shape[0]
        blocks += [first + i for i in range(g.shape[0])]
    block = pl.BlockSpec((1, rows, ff), lambda i, ls, rs: (ls[i], rs[i], 0))

    def part_spec(s):
        shape = parts[s][0].shape
        return pl.BlockSpec((1, *shape[1:]), lambda i, ls, rs: (jnp.clip(i - starts[s], 0, shape[0] - 1), 0, 0, 0, 0))

    size = 2 * starts[-1] * rows * ff
    return pl.pallas_call(
        functools.partial(wide_kernel, starts),
        grid_spec=pltpu.PrefetchScalarGridSpec(
            num_scalar_prefetch=2,
            grid=(starts[-1],),
            in_specs=[pl.BlockSpec((8, LANES), lambda i, ls, rs: (0, 0))] + [part_spec(s) for s in range(len(parts))] + [block] * 6 + [ANY] * len(before),
            out_specs=[block] * 6,
        ),
        out_shape=[jax.ShapeDtypeStruct(a.shape, a.dtype) for a in arrays],
        input_output_aliases={3 + len(parts) + 6 + i: i for i in range(len(before))},
        compiler_params=pltpu.CompilerParams(vmem_limit_bytes=62 * 2**20),
        cost_estimate=pl.CostEstimate(flops=1000 * size, bytes_accessed=22 * size, transcendentals=size),
        name="update_wide",
    )(jnp.array(layers, jnp.int32), jnp.stack(blocks).astype(jnp.int32), f, *(g for g, _, _ in parts), *arrays, *before)


def tall_kernel(count, row_of, f_ref, *refs):
    parts, (w, m, v, nw, nm, nv, whole) = refs[:count], refs[count:]
    f = f_ref[0:1, 0:1]
    for s, part in enumerate(parts):
        rows = part.shape[0] * part.shape[2]
        whole[pl.ds(pl.multiple_of(row_of[s], 8), rows), :] = part[:, 0].astype(F32).reshape(rows, BLOCK)
    for at in range(0, BLOCK, LANES):
        rows = slice(at, at + LANES)
        g = whole[:, rows].T
        nw[0, rows, :], nm[0, rows, :], nv[0, rows, :] = adamw(f, g, w[0, rows, :], m[0, rows, :], v[0, rows, :])


def update_tall(f, parts, w, m, v):
    layers, ff, d = w.shape
    nb = ff // BLOCK
    block = pl.BlockSpec((1, BLOCK, d), lambda c, rs: (layers - 1 - c // nb, c % nb, 0))
    size = layers * d * ff
    return pl.pallas_call(
        functools.partial(tall_kernel, len(parts)),
        grid_spec=pltpu.PrefetchScalarGridSpec(
            num_scalar_prefetch=1,
            grid=(layers * nb,),
            in_specs=[pl.BlockSpec((8, LANES), lambda c, rs: (0, 0))]
            + [pl.BlockSpec((g.shape[0], 1, *g.shape[2:]), lambda c, rs: (0, c, 0, 0)) for g, _ in parts]
            + [block] * 3,
            out_specs=[block] * 3,
            scratch_shapes=[pltpu.VMEM((d, BLOCK), F32)],
        ),
        out_shape=[jax.ShapeDtypeStruct(a.shape, a.dtype) for a in (w, m, v)],
        compiler_params=pltpu.CompilerParams(vmem_limit_bytes=62 * 2**20),
        cost_estimate=pl.CostEstimate(flops=1000 * size, bytes_accessed=22 * size, transcendentals=size),
        name="update_tall",
    )(jnp.stack([row for _, row in parts]).astype(jnp.int32), f, *(g for g, _ in parts), w, m, v)


def solution(mesh):
    n = mesh.shape["dp"]
    side = math.isqrt(n)
    along = lambda h, i, step: ((i // side + step) % side) * side + i % side if h == 0 else i // side * side + (i + step) % side

    def move(array, h, step):
        return lax.ppermute(array, "dp", [(i, along(h, i, step)) for i in range(n)])

    def near(sets):
        return [move(mine, h, to) for h, mine in enumerate(sets) for to in (1, -1)]

    def halves(sets):
        return [part[: side // 2] if i % 2 == 0 else part[side // 2 :] for i, part in enumerate(sets)]

    def far(parts):
        return [move(part, i // 2, 1 - 2 * (i % 2)) for i, part in enumerate(parts)]

    def step(x, dy, wg, wu, wd, mg, mu, md, vg, vu, vd):
        a, at, h, dyt = forward(x, dy, wg, wu, wd)
        set_d, set_gu, f = backward(side, float(wg.size + wu.size + wd.size), a, at, h, dy, dyt, wg, wu, wd)
        pr = set_d[0].shape[2]
        p = [spot[0] for spot in places(side)]
        own_rows = [(h * side + p[h]) * side for h in range(2)]
        near_rows = [(h * side + (p[h] + side - to) % side) * side for h in range(2) for to in (1, -1)]
        far_rows = [(h * side + (p[h] + 2) % side) * side + way * (side // 2) for h in range(2) for way in range(2)]
        arrays = (wg, wu, mg, mu, vg, vu)
        wide = lambda sets, rows, before: update_wide(f, [(g, l, row) for l, gs in sets for g, row in zip(gs, rows, strict=True)], arrays, before)

        near_d = near(set_d)
        new = wide([(1, set_gu[1])], own_rows, ())
        half_d, new = lax.optimization_barrier((halves(near_d), new))
        far_d = far(half_d)
        new = wide([(0, set_gu[0])], own_rows, new)
        far_d, set_gu, new = lax.optimization_barrier((far_d, set_gu, new))
        near_gu = {l: near(set_gu[l]) for l in (1, 0)}
        parts = [*zip(set_d, own_rows), *zip(near_d, near_rows), *zip(far_d, far_rows)]
        tall = update_tall(f, [(g, row * pr) for g, row in parts], wd, md, vd)
        near_gu, tall, new = lax.optimization_barrier((near_gu, tall, new))
        far_gu = {l: far(halves(near_gu[l])) for l in (1, 0)}
        for l in (1, 0):
            new = wide([(l, near_gu[l])], near_rows, new)
        for l in (1, 0):
            new = wide([(l, far_gu[l])], far_rows, new)
        return new[0], new[1], tall[0], new[2], new[3], tall[1], new[4], new[5], tall[2]

    return jax.shard_map(
        step,
        mesh=mesh,
        in_specs=(P(("rep", "dp"), None, None),) * 2 + (P(None, None, None),) * 9,
        out_specs=(P("rep", None, None),) * 9,
        check_vma=False,
    )
```

```python
import functools
import math

import jax
import jax.numpy as jnp
from jax import lax
from jax.experimental import pallas as pl
from jax.experimental.pallas import tpu as pltpu
from jax.sharding import PartitionSpec as P

MESH = pl.DeviceIdType.MESH
BLOCK = 256
LANES = 128
LAG = 2
SLOTS = 2 * LAG + 2
SENT = LAG + 1
BF16, F32 = jnp.bfloat16, jnp.float32
ANY = pl.BlockSpec(memory_space=pl.ANY)
VMEM = pl.BlockSpec(memory_space=pltpu.VMEM)


def dot(a, b, over=((1,), (0,))):
    return lax.dot_general(a, b, (over, ((), ())), preferred_element_type=F32)


def sigmoid(v):
    return 0.5 + 0.5 * jnp.tanh(0.5 * v)


def normed(wide):
    return (wide * lax.rsqrt(jnp.mean(wide * wide, -1, keepdims=True) + 1e-6)).astype(BF16)


def forward_kernel(x_ref, dy_ref, wg_ref, wu_ref, wd_ref, a_ref, at_ref, h_ref, dyt_ref, act):
    rows = x_ref.shape[1] // 2
    for t in range(2):
        at = slice(t * rows, (t + 1) * rows)
        x = x_ref[0, at].astype(F32)
        a = normed(x)
        a_ref[0, at] = a
        at_ref[0, :, at] = a.T
        for b in range(wg_ref.shape[2] // BLOCK):
            cols = slice(b * BLOCK, (b + 1) * BLOCK)
            gate, up = dot(a, wg_ref[0, :, cols]), dot(a, wu_ref[0, :, cols])
            act[at, cols] = (gate * sigmoid(gate) * up).astype(BF16)
        dyt_ref[:, at] = dy_ref[0, at].T
        h = (x + dot(act[at, :], wd_ref[0]).astype(BF16).astype(F32)).astype(BF16)
        h_ref[at, :] = h
        a = normed(h.astype(F32))
        a_ref[1, at] = a
        at_ref[1, :, at] = a.T


def forward(x, dy, wg, wu, wd):
    _, tokens, d = x.shape
    ff = wg.shape[2]
    rows = min(512, tokens)
    tall = pl.BlockSpec((1, rows, d), lambda i: (0, i, 0))
    out = [((2, tokens, d), (2, rows, d), lambda i: (0, i, 0)), ((2, d, tokens), (2, d, rows), lambda i: (0, 0, i))]
    out += [((tokens, d), (rows, d), lambda i: (i, 0)), ((d, tokens), (d, rows), lambda i: (0, i))]
    return pl.pallas_call(
        forward_kernel,
        grid=(tokens // rows,),
        out_shape=[jax.ShapeDtypeStruct(s, BF16) for s, _, _ in out],
        in_specs=[tall, tall]
        + [pl.BlockSpec((1, *w.shape[1:]), lambda i: (0, 0, 0), pipeline_mode=pl.Buffered(1)) for w in (wg, wu, wd)],
        out_specs=[pl.BlockSpec(b, m) for _, b, m in out],
        scratch_shapes=[pltpu.VMEM((rows, ff), BF16)],
        compiler_params=pltpu.CompilerParams(vmem_limit_bytes=60 * 2**20),
        cost_estimate=pl.CostEstimate(flops=6 * tokens * d * ff, bytes_accessed=2 * (9 * tokens * d + 3 * d * ff), transcendentals=tokens * ff),
        name="forward",
    )(x, dy, wg, wu, wd)


def places(side):
    me = lax.axis_index("dp")
    x, y = me // side, me % side
    along_x = lambda d: lax.rem(x + side + d, side) * side + y
    along_y = lambda d: x * side + lax.rem(y + side + d, side)
    return ((x, y, along_x, along_y), (y, x, along_y, along_x))


def backward_kernel(side, count, a_hbm, at_hbm, h_hbm, dy_hbm, dyt_hbm, wg_hbm, wu_hbm, wd_hbm, *refs):
    set_d, set_gu, f_ref, scratch = refs[0:2], (refs[2:4], refs[4:6]), refs[6], refs[7:]
    (A, AT, H, DY, DYT, ACT, DG, DU, WB, WD, WG1, WU1, TERM, R1, R2, R3, R4, ACC, SA, SB, OWN, SQ, MINE, SQS) = scratch[:-6]
    load_sems, w_sems, send_sems, recv_sems, own_sems, sq_sems = scratch[-6:]
    tokens, d = A.shape
    ff = DG.shape[1]
    nb = ff // BLOCK
    chunks = 2 * nb
    rows = min(512, tokens)
    n = side * side
    me = lax.axis_index("dp")
    pr = d // (2 * n)
    spots = places(side)
    wrap = lambda v: lax.rem(v, side)

    def remote(src, dst, stage, slot, h, way, to):
        return pltpu.make_async_remote_copy(
            src_ref=src, dst_ref=dst, send_sem=send_sems.at[stage, slot, h, way], recv_sem=recv_sems.at[stage, slot, h, way],
            device_id={"dp": to}, device_id_type=MESH,
        )

    def message(stage, slot, h, way):
        p, q, to_p, to_q = spots[h]
        step = 1 - 2 * way
        if stage == 0:
            return remote(TERM.at[slot, h, wrap(p + 2), pl.ds(2 * way, 2)], R1.at[slot, h, way], 0, slot, h, way, to_p(step))
        if stage == 1:
            return remote(TERM.at[slot, h, wrap(p + side + step)], R2.at[slot, h, way], 1, slot, h, way, to_p(step))
        if stage == 2:
            part = pl.ds(2 * way, 2 - way)
            return remote(SA.at[slot % SENT, h, part], R3.at[slot, h, part], 2, slot, h, way, to_q(step))
        return remote(SB.at[slot % SENT, h, way], R4.at[slot, h, way], 3, slot, h, way, to_q(step))

    def both(stage, slot, h, what):
        for way in range(2):
            getattr(message(stage, slot, h, way), what)()

    def stage0(c):
        for h in range(2):
            both(0, c % SLOTS, h, "start")

    def stage1(c):
        slot = c % SLOTS
        for h in range(2):
            p = spots[h][0]
            both(0, slot, h, "wait_recv")
            both(0, slot, h, "wait_send")
            for way, at in ((0, wrap(p + 1)), (1, wrap(p + side - 1))):
                half = pl.ds(2 * way, 2)
                TERM[slot, h, at, half] = (TERM[slot, h, at, half].astype(F32) + R1[slot, h, way].astype(F32)).astype(BF16)
            both(1, slot, h, "start")

    def stage2(c):
        slot = c % SLOTS
        for h in range(2):
            p, q = spots[h][:2]
            both(1, slot, h, "wait_recv")
            both(1, slot, h, "wait_send")
            for o in range(side):
                ACC[slot, h, o] = TERM[slot, h, p, o].astype(F32) + R2[slot, h, 0, o].astype(F32) + R2[slot, h, 1, o].astype(F32)
            SA[slot % SENT, h] = ACC[slot, h, wrap(q + 2)].astype(BF16)
            both(2, slot, h, "start")

    def stage3(c):
        slot = c % SLOTS
        for h in range(2):
            q = spots[h][1]
            both(2, slot, h, "wait_recv")
            both(2, slot, h, "wait_send")
            after, before = wrap(q + 1), wrap(q + side - 1)
            SB[slot % SENT, h, 0, 0:2] = (ACC[slot, h, after, 0:2] + R3[slot, h, 0:2].astype(F32)).astype(BF16)
            SB[slot % SENT, h, 0, 2:3] = ACC[slot, h, after, 2:3].astype(BF16)
            SB[slot % SENT, h, 1, 0:2] = ACC[slot, h, before, 0:2].astype(BF16)
            SB[slot % SENT, h, 1, 2:3] = (ACC[slot, h, before, 2:3] + R3[slot, h, 2:3].astype(F32)).astype(BF16)
            both(3, slot, h, "start")

    def by_layer(c, do):
        for l in range(2):
            pl.when(c // nb == 1 - l)(functools.partial(do, l))

    def gather_message(part, l, slot, h, way, c):
        q, to_q = spots[h][1], spots[h][3]
        step = 1 - 2 * way
        at = q if part < 2 else wrap(q + side - step)
        dst = set_gu[l][h].at[at, c % nb] if part % 2 == 0 else set_d[h].at[at, c]
        src = (OWN.at[slot % SENT, h, pl.ds(0, 2)] if part == 0 else OWN.at[slot % SENT, h, 2]) if part < 2 else dst
        return remote(src, dst, 4 + part, slot, h, way, to_q(step))

    def own_copy(part, l, slot, h, c):
        q = spots[h][1]
        if part == 0:
            return pltpu.make_async_copy(OWN.at[slot % SENT, h, pl.ds(0, 2)], set_gu[l][h].at[q, c % nb], own_sems.at[slot, h, 0])
        return pltpu.make_async_copy(OWN.at[slot % SENT, h, 2], set_d[h].at[q, c], own_sems.at[slot, h, 1])

    def stage4(c):
        slot = c % SLOTS
        for h in range(2):
            q = spots[h][1]
            both(3, slot, h, "wait_recv")
            both(3, slot, h, "wait_send")
            g = (ACC[slot, h, q] + R4[slot, h, 0].astype(F32) + R4[slot, h, 1].astype(F32)).astype(BF16)
            OWN[slot % SENT, h] = g
            g = g.astype(F32)
            SQ[...] += g[0] * g[0] + g[1] * g[1] + g[2] * g[2]

            def gate_up(l, h=h):
                own_copy(0, l, slot, h, c).start()
                for way in range(2):
                    gather_message(0, l, slot, h, way, c).start()

            by_layer(c, gate_up)
            own_copy(1, 0, slot, h, c).start()
            for way in range(2):
                gather_message(1, 0, slot, h, way, c).start()

    def stage5(c):
        slot = c % SLOTS
        for h in range(2):
            for part in range(2):
                for way in range(2):
                    copy = gather_message(part, 0, slot, h, way, c)
                    copy.wait_recv()
                    copy.wait_send()
                own_copy(part, 0, slot, h, c).wait()
            by_layer(c, lambda l, h=h: gather_message(2, l, slot, h, 0, c).start())
            gather_message(3, 0, slot, h, 1, c).start()

    def stage6(c):
        slot = c % SLOTS
        for h in range(2):
            for part, way in ((2, 0), (3, 1)):
                copy = gather_message(part, 0, slot, h, way, c)
                copy.wait_recv()
                copy.wait_send()

    def square(d):
        return pltpu.make_async_remote_copy(
            src_ref=MINE, dst_ref=SQS.at[me], send_sem=sq_sems.at[0, d], recv_sem=sq_sems.at[1, d],
            device_id={"dp": lax.rem(me + d, n)}, device_id_type=MESH,
        )

    def squares():
        total = jnp.broadcast_to(jnp.sum(SQ[...], axis=0, keepdims=True), MINE.shape)
        MINE[...] = total
        SQS[me] = total
        for d in range(1, n):
            square(d).start()

    def load(which, l=1):
        src, dst = {"A": (a_hbm.at[l], A), "AT": (at_hbm.at[l], AT), "H": (h_hbm, H), "DY": (dy_hbm.at[0], DY), "DYT": (dyt_hbm, DYT),
                    "WG1": (wg_hbm.at[1], WG1), "WU1": (wu_hbm.at[1], WU1)}[which]
        return pltpu.make_async_copy(src, dst, load_sems.at[("A", "AT", "H", "DY", "DYT", "WG1", "WU1").index(which)])

    def weights(i, what):
        l, at, slot = 1 - i // nb, pl.multiple_of((i % nb) * BLOCK, BLOCK), i % 2
        for j, (src, dst) in enumerate((
            (wg_hbm.at[l, :, pl.ds(at, BLOCK)], WB.at[slot, 0]),
            (wu_hbm.at[l, :, pl.ds(at, BLOCK)], WB.at[slot, 1]),
            (wd_hbm.at[l, pl.ds(at, BLOCK), :], WD.at[slot]),
        )):
            getattr(pltpu.make_async_copy(src, dst, w_sems.at[slot, j]), what)()

    def middle():
        load("A", 0).start()
        load("AT", 0).start()
        for which in ("H", "WG1", "WU1"):
            load(which).wait()
        for t in range(tokens // rows):
            at = slice(t * rows, (t + 1) * rows)
            by_a = dot(DG[at, :], WG1[...], ((1,), (1,))).astype(BF16).astype(F32)
            by_a = (by_a + dot(DU[at, :], WU1[...], ((1,), (1,))).astype(BF16).astype(F32)).astype(BF16).astype(F32)
            wide = H[at, :].astype(F32)
            scale = lax.rsqrt(jnp.mean(wide * wide, -1, keepdims=True) + 1e-6)
            by_scale = jnp.sum(by_a * wide, -1, keepdims=True)
            by_wide = (by_a * scale - wide * (by_scale * scale * scale * scale * (1.0 / d))).astype(BF16).astype(F32)
            by_h = (DY[at, :].astype(F32) + by_wide).astype(BF16)
            DY[at, :] = by_h
            DYT[:, at] = by_h.T
        load("A", 0).wait()
        load("AT", 0).wait()

    def compute(i):
        slot, ws = i % SLOTS, i % 2
        cols = pl.ds(pl.multiple_of((i % nb) * BLOCK, BLOCK), BLOCK)
        weights(i, "wait")

        @pl.when(i + 1 < chunks)
        def _():
            weights(i + 1, "start")

        for t in range(tokens // rows):
            at = slice(t * rows, (t + 1) * rows)
            gate, up = dot(A[at, :], WB[ws, 0]), dot(A[at, :], WB[ws, 1])
            by_act = dot(DY[at, :], WD[ws], ((1,), (1,))).astype(BF16).astype(F32)
            sig = sigmoid(gate)
            silu = gate * sig
            ACT[at, :] = (silu * up).astype(BF16)
            DU[at, cols] = (by_act * silu).astype(BF16)
            DG[at, cols] = (by_act * up * (sig * (1.0 + gate * (1.0 - sig)))).astype(BF16)

        @pl.when(i == 0)
        def _():
            load("AT").wait()
            load("DYT").wait()

        for j, (left, right) in enumerate(((AT, DG[:, cols]), (AT, DU[:, cols]), (DYT, ACT[...]))):
            g = dot(left[...], right)
            for o in range(2 * side):
                piece = g[o * side * pr : (o + 1) * side * pr].reshape(side, pr, BLOCK)
                TERM[slot, o // side, o % side, :, j] = piece.astype(BF16)

    for which in ("A", "DY", "AT", "DYT", "H", "WG1", "WU1"):
        load(which).start()
    weights(0, "start")
    barrier = pltpu.get_barrier_semaphore()
    for other in range(1, n):
        pl.semaphore_signal(barrier, inc=1, device_id={"dp": lax.rem(me + other, n)}, device_id_type=MESH)
    SQ[...] = jnp.zeros_like(SQ)
    load("A").wait()
    load("DY").wait()
    pl.semaphore_wait(barrier, n - 1)

    @pl.loop(0, chunks + 6 * LAG)
    def _(i):
        pl.when(i == nb)(middle)
        pl.when(i < chunks)(lambda: compute(i))
        pl.when(i < chunks)(lambda: stage0(i))
        for lag, stage in enumerate((stage1, stage2, stage3, stage4, stage5, stage6), 1):
            late = lag * LAG
            pl.when((i >= late) & (i < chunks + late))(functools.partial(stage, i - late))
        pl.when(i == chunks - 1 + 4 * LAG)(squares)

    for other in range(1, n):
        square(other).wait_recv()
    for other in range(1, n):
        square(other).wait_send()
    total = jnp.zeros(MINE.shape, F32)
    for device in range(n):
        total = total + SQS[device]
    total = jnp.sum(total[0:1], axis=1, keepdims=True)
    f_ref[...] = jnp.broadcast_to(jnp.minimum(1.0, 0.5 * lax.rsqrt(total / count + 1e-30)), f_ref.shape)


def backward(side, count, a, at, h, dy, dyt, wg, wu, wd):
    _, tokens, d = a.shape
    ff = wg.shape[2]
    nb = ff // BLOCK
    pr = d // (2 * side**2)
    piece = (3, pr, BLOCK)
    v = pltpu.VMEM
    sems = pltpu.SemaphoreType.DMA
    shapes = [(side, 2 * nb, pr, BLOCK)] * 2 + [(side, nb, 2, pr, BLOCK)] * 4
    out = pl.pallas_call(
        functools.partial(backward_kernel, side, count),
        out_shape=[jax.ShapeDtypeStruct(s, BF16) for s in shapes] + [jax.ShapeDtypeStruct((8, LANES), F32)],
        in_specs=[ANY] * 8,
        out_specs=[ANY] * 6 + [VMEM],
        scratch_shapes=[
            v((tokens, d), BF16), v((d, tokens), BF16), v((tokens, d), BF16), v((tokens, d), BF16), v((d, tokens), BF16),
            v((tokens, BLOCK), BF16), v((tokens, ff), BF16), v((tokens, ff), BF16),
            v((2, 2, d, BLOCK), BF16), v((2, BLOCK, d), BF16), v((d, ff), BF16), v((d, ff), BF16),
            v((SLOTS, 2, side, side, *piece), BF16), v((SLOTS, 2, 2, 2, *piece), BF16), v((SLOTS, 2, 2, side, *piece), BF16),
            v((SLOTS, 2, *piece), BF16), v((SLOTS, 2, 2, *piece), BF16), v((SLOTS, 2, side, *piece), F32),
            v((SENT, 2, *piece), BF16), v((SENT, 2, 2, *piece), BF16), v((SENT, 2, *piece), BF16),
            v((pr, BLOCK), F32), v((8, BLOCK), F32), v((side**2, 8, BLOCK), F32),
            sems((7,)), sems((2, 3)), sems((8, SLOTS, 2, 2)), sems((8, SLOTS, 2, 2)), sems((SLOTS, 2, 2)), sems((2, side**2)),
        ],
        compiler_params=pltpu.CompilerParams(collective_id=0, has_side_effects=True, vmem_limit_bytes=67043328),
        cost_estimate=pl.CostEstimate(flops=28 * tokens * d * ff, bytes_accessed=2 * (7 * tokens * d + 8 * d * ff), transcendentals=2 * tokens * ff),
        name="backward",
    )(a, at, h, dy, dyt, wg, wu, wd)
    return out[0:2], (out[2:4], out[4:6]), out[6]


def adamw(f, g, w, m, v):
    g = g.astype(F32) * f
    m = 0.9 * m + 0.1 * g
    v = 0.95 * v + 0.05 * g * g
    w = w.astype(F32)
    return (w - 0.02 * (m * lax.rsqrt(v + 1e-8) + 0.1 * w)).astype(BF16), m, v


STEP = 2


def wide_kernel(count, table, f_ref, *refs):
    parts, ins, outs = refs[:count], refs[count : count + 6], refs[-6:]
    f = f_ref[0:1, 0:1]
    per = 4 // STEP
    step = pl.program_id(0)
    for s in range(count):

        @pl.when(step // per == s)
        def _(part=parts[s]):
            _, nb, _, pr, _ = part.shape
            for j in range(2):
                w, m, v = ins[j::2]
                nw, nm, nv = outs[j::2]
                for b in range(nb):
                    cols = slice(b * BLOCK, (b + 1) * BLOCK)
                    for q in range(STEP):
                        at = slice(q * pr, (q + 1) * pr)
                        nw[0, at, cols], nm[0, at, cols], nv[0, at, cols] = adamw(f, part[q, b, j], w[0, at, cols], m[0, at, cols], v[0, at, cols])


def update_wide(table, f, parts, arrays, before):
    _, _, ff = arrays[0].shape
    side, _, _, pr, _ = parts[0][0].shape
    per = side // STEP

    def pick(i, values):
        which, chosen = i // per, values[-1]
        for s in range(len(values) - 2, -1, -1):
            chosen = jnp.where(which == s, values[s], chosen)
        return chosen

    layers, indices = [l for _, l, _ in parts], [index for _, _, index in parts]
    block = pl.BlockSpec((1, STEP * pr, ff), lambda i, table: (pick(i, layers), table[pick(i, indices)] * per + i % per, 0))

    def part_spec(s):
        shape = parts[s][0].shape
        return pl.BlockSpec((STEP, *shape[1:]), lambda i, table: (jnp.clip(i - s * per, 0, per - 1), 0, 0, 0, 0))

    size = 2 * len(parts) * side * pr * ff
    return pl.pallas_call(
        functools.partial(wide_kernel, len(parts)),
        grid_spec=pltpu.PrefetchScalarGridSpec(
            num_scalar_prefetch=1,
            grid=(len(parts) * per,),
            in_specs=[pl.BlockSpec((8, LANES), lambda i, table: (0, 0))] + [part_spec(s) for s in range(len(parts))] + [block] * 6 + [ANY] * len(before),
            out_specs=[block] * 6,
        ),
        out_shape=[jax.ShapeDtypeStruct(a.shape, a.dtype) for a in arrays],
        input_output_aliases={2 + len(parts) + 6 + i: i for i in range(len(before))},
        compiler_params=pltpu.CompilerParams(vmem_limit_bytes=62 * 2**20),
        cost_estimate=pl.CostEstimate(flops=1000 * size, bytes_accessed=22 * size, transcendentals=size),
        name="update_wide",
    )(table, f, *(g for g, _, _ in parts), *arrays, *before)


def tall_kernel(indices, table, f_ref, *refs):
    count = len(indices)
    parts, (w, m, v, nw, nm, nv, whole) = refs[:count], refs[count:]
    f = f_ref[0:1, 0:1]
    for s, part in enumerate(parts):
        rows = part.shape[0] * part.shape[2]
        index, first = indices[s]
        whole[pl.ds(pl.multiple_of(table[index] * (4 * part.shape[2]) + first * part.shape[2], 8), rows), :] = part[:, 0].astype(F32).reshape(rows, BLOCK)
    for at in range(0, BLOCK, LANES):
        rows = slice(at, at + LANES)
        g = whole[:, rows].T
        nw[0, rows, :], nm[0, rows, :], nv[0, rows, :] = adamw(f, g, w[0, rows, :], m[0, rows, :], v[0, rows, :])


def update_tall(table, f, parts, w, m, v):
    layers, ff, d = w.shape
    nb = ff // BLOCK
    block = pl.BlockSpec((1, BLOCK, d), lambda c, table: (layers - 1 - c // nb, c % nb, 0))
    size = layers * d * ff
    return pl.pallas_call(
        functools.partial(tall_kernel, [(index, first) for _, index, first in parts]),
        grid_spec=pltpu.PrefetchScalarGridSpec(
            num_scalar_prefetch=1,
            grid=(layers * nb,),
            in_specs=[pl.BlockSpec((8, LANES), lambda c, table: (0, 0))]
            + [pl.BlockSpec((g.shape[0], 1, *g.shape[2:]), lambda c, table: (0, c, 0, 0)) for g, _, _ in parts]
            + [block] * 3,
            out_specs=[block] * 3,
            scratch_shapes=[pltpu.VMEM((d, BLOCK), F32)],
        ),
        out_shape=[jax.ShapeDtypeStruct(a.shape, a.dtype) for a in (w, m, v)],
        compiler_params=pltpu.CompilerParams(vmem_limit_bytes=62 * 2**20),
        cost_estimate=pl.CostEstimate(flops=1000 * size, bytes_accessed=22 * size, transcendentals=size),
        name="update_tall",
    )(table, f, *(g for g, _, _ in parts), w, m, v)


def solution(mesh):
    n = mesh.shape["dp"]
    side = math.isqrt(n)
    along = lambda h, i, step: ((i // side + step) % side) * side + i % side if h == 0 else i // side * side + (i + step) % side

    def move(array, h, step):
        return lax.ppermute(array, "dp", [(i, along(h, i, step)) for i in range(n)])

    def near(sets):
        return [move(mine, h, to) for h, mine in enumerate(sets) for to in (1, -1)]

    def halves(sets):
        return [part[: side // 2] if i % 2 == 0 else part[side // 2 :] for i, part in enumerate(sets)]

    def far(parts):
        return [move(part, i // 2, 1 - 2 * (i % 2)) for i, part in enumerate(parts)]

    def step(x, dy, wg, wu, wd, mg, mu, md, vg, vu, vd):
        a, at, h, dyt = forward(x, dy, wg, wu, wd)
        set_d, set_gu, f = backward(side, float(wg.size + wu.size + wd.size), a, at, h, dy, dyt, wg, wu, wd)
        p = [spot[0] for spot in places(side)]
        table = [h * side + p[h] for h in range(2)]
        table += [h * side + (p[h] + side - to) % side for h in range(2) for to in (1, -1)]
        table += [h * side + (p[h] + 2) % side for h in range(2)]
        table = jnp.stack(table).astype(jnp.int32)
        arrays = (wg, wu, mg, mu, vg, vu)
        wide = lambda parts, before: update_wide(table, f, parts, arrays, before)

        near_d = near(set_d)
        new = wide([(set_gu[1][h], 1, h) for h in range(2)], ())
        half_d, new = lax.optimization_barrier((halves(near_d), new))
        far_d = far(half_d)
        new = wide([(set_gu[0][h], 0, h) for h in range(2)], new)
        far_d, set_gu, new = lax.optimization_barrier((far_d, set_gu, new))
        near_gu = {l: near(set_gu[l]) for l in (1, 0)}
        parts = [(set_d[h], h, 0) for h in range(2)] + [(g, 2 + i, 0) for i, g in enumerate(near_d)]
        parts += [(g, 6 + i // 2, (i % 2) * (side // 2)) for i, g in enumerate(far_d)]
        tall = update_tall(table, f, parts, wd, md, vd)
        near_gu, tall, new = lax.optimization_barrier((near_gu, tall, new))
        far_gu = [(move(near_gu[l][2 * h + 1 - l], h, 2 * l - 1), l, 6 + h) for l in (1, 0) for h in range(2)]
        for l in (1, 0):
            new = wide([(g, l, 2 + i) for i, g in enumerate(near_gu[l])], new)
        new = wide(far_gu, new)
        return new[0], new[1], tall[0], new[2], new[3], tall[1], new[4], new[5], tall[2]

    return jax.shard_map(
        step,
        mesh=mesh,
        in_specs=(P(("rep", "dp"), None, None),) * 2 + (P(None, None, None),) * 9,
        out_specs=(P("rep", None, None),) * 9,
        check_vma=False,
    )
```

```python
import functools
import math

import jax
import jax.numpy as jnp
from jax import lax
from jax.experimental import pallas as pl
from jax.experimental.pallas import tpu as pltpu
from jax.sharding import PartitionSpec as P

MESH = pl.DeviceIdType.MESH
BLOCK = 256
LANES = 128
LAG = 2
SLOTS = 2 * LAG + 2
SENT = LAG + 1
BF16, F32 = jnp.bfloat16, jnp.float32
ANY = pl.BlockSpec(memory_space=pl.ANY)
VMEM = pl.BlockSpec(memory_space=pltpu.VMEM)


def dot(a, b, over=((1,), (0,))):
    return lax.dot_general(a, b, (over, ((), ())), preferred_element_type=F32)


def sigmoid(v):
    return 0.5 + 0.5 * jnp.tanh(0.5 * v)


def normed(wide):
    return (wide * lax.rsqrt(jnp.mean(wide * wide, -1, keepdims=True) + 1e-6)).astype(BF16)


def forward_kernel(x_ref, dy_ref, wg_ref, wu_ref, wd_ref, a_ref, at_ref, h_ref, dyt_ref, act):
    rows = x_ref.shape[1] // 2
    for t in range(2):
        at = slice(t * rows, (t + 1) * rows)
        x = x_ref[0, at].astype(F32)
        a = normed(x)
        a_ref[0, at] = a
        at_ref[0, :, at] = a.T
        for b in range(wg_ref.shape[2] // BLOCK):
            cols = slice(b * BLOCK, (b + 1) * BLOCK)
            gate, up = dot(a, wg_ref[0, :, cols]), dot(a, wu_ref[0, :, cols])
            act[at, cols] = (gate * sigmoid(gate) * up).astype(BF16)
        dyt_ref[:, at] = dy_ref[0, at].T
        h = (x + dot(act[at, :], wd_ref[0]).astype(BF16).astype(F32)).astype(BF16)
        h_ref[at, :] = h
        a = normed(h.astype(F32))
        a_ref[1, at] = a
        at_ref[1, :, at] = a.T


def forward(x, dy, wg, wu, wd):
    _, tokens, d = x.shape
    ff = wg.shape[2]
    rows = min(512, tokens)
    tall = pl.BlockSpec((1, rows, d), lambda i: (0, i, 0))
    out = [((2, tokens, d), (2, rows, d), lambda i: (0, i, 0)), ((2, d, tokens), (2, d, rows), lambda i: (0, 0, i))]
    out += [((tokens, d), (rows, d), lambda i: (i, 0)), ((d, tokens), (d, rows), lambda i: (0, i))]
    return pl.pallas_call(
        forward_kernel,
        grid=(tokens // rows,),
        out_shape=[jax.ShapeDtypeStruct(s, BF16) for s, _, _ in out],
        in_specs=[tall, tall]
        + [pl.BlockSpec((1, *w.shape[1:]), lambda i: (0, 0, 0), pipeline_mode=pl.Buffered(1)) for w in (wg, wu, wd)],
        out_specs=[pl.BlockSpec(b, m) for _, b, m in out],
        scratch_shapes=[pltpu.VMEM((rows, ff), BF16)],
        compiler_params=pltpu.CompilerParams(vmem_limit_bytes=60 * 2**20),
        cost_estimate=pl.CostEstimate(flops=6 * tokens * d * ff, bytes_accessed=2 * (9 * tokens * d + 3 * d * ff), transcendentals=tokens * ff),
        name="forward",
    )(x, dy, wg, wu, wd)


def places(side):
    me = lax.axis_index("dp")
    x, y = me // side, me % side
    along_x = lambda d: lax.rem(x + side + d, side) * side + y
    along_y = lambda d: x * side + lax.rem(y + side + d, side)
    return ((x, y, along_x, along_y), (y, x, along_y, along_x))


def backward_kernel(side, count, a_hbm, at_hbm, h_hbm, dy_hbm, dyt_hbm, wg_hbm, wu_hbm, wd_hbm, *refs):
    set_d, set_gu, f_ref, scratch = refs[0:2], (refs[2:4], refs[4:6]), refs[6], refs[7:]
    (A, AT, H, DY, DYT, ACT, DG, DU, WB, WD, WG1, WU1, TERM, R1, R2, R3, R4, ACC, SA, SB, OWN, SQ, MINE, SQS) = scratch[:-6]
    load_sems, w_sems, send_sems, recv_sems, own_sems, sq_sems = scratch[-6:]
    tokens, d = A.shape
    ff = DG.shape[1]
    nb = ff // BLOCK
    chunks = 2 * nb
    rows = min(512, tokens)
    n = side * side
    me = lax.axis_index("dp")
    pr = d // (2 * n)
    spots = places(side)
    wrap = lambda v: lax.rem(v, side)

    def remote(src, dst, stage, slot, to):
        return pltpu.make_async_remote_copy(
            src_ref=src, dst_ref=dst, send_sem=send_sems.at[stage, slot], recv_sem=recv_sems.at[stage, slot],
            device_id={"dp": to}, device_id_type=MESH,
        )

    def settle(stage, slot, like):
        copy = remote(like, like, stage, slot, me)
        copy.wait_recv()
        copy.wait_send()

    def message(stage, slot, h, way):
        p, q, to_p, to_q = spots[h]
        step = 1 - 2 * way
        if stage == 0:
            return remote(TERM.at[slot, h, wrap(p + 2), pl.ds(2 * way, 2)], R1.at[slot, h, way], 0, slot, to_p(step))
        if stage == 1:
            return remote(TERM.at[slot, h, wrap(p + side + step)], R2.at[slot, h, way], 1, slot, to_p(step))
        if stage == 2:
            part = pl.ds(2 * way, 2 - way)
            return remote(SA.at[slot % SENT, h, part], R3.at[slot, h, part], 2, slot, to_q(step))
        return remote(SB.at[slot % SENT, h, way], R4.at[slot, h, way], 3, slot, to_q(step))

    def both(stage, slot, h):
        for way in range(2):
            message(stage, slot, h, way).start()

    def stage0(c):
        for h in range(2):
            both(0, c % SLOTS, h)

    def stage1(c):
        slot = c % SLOTS
        settle(0, slot, R1.at[slot])
        for h in range(2):
            p = spots[h][0]
            for way, at in ((0, wrap(p + 1)), (1, wrap(p + side - 1))):
                half = pl.ds(2 * way, 2)
                TERM[slot, h, at, half] = (TERM[slot, h, at, half].astype(F32) + R1[slot, h, way].astype(F32)).astype(BF16)
            both(1, slot, h)

    def stage2(c):
        slot = c % SLOTS
        settle(1, slot, R2.at[slot])
        for h in range(2):
            p, q = spots[h][:2]
            for o in range(side):
                ACC[slot, h, o] = TERM[slot, h, p, o].astype(F32) + R2[slot, h, 0, o].astype(F32) + R2[slot, h, 1, o].astype(F32)
            SA[slot % SENT, h] = ACC[slot, h, wrap(q + 2)].astype(BF16)
            both(2, slot, h)

    def stage3(c):
        slot = c % SLOTS
        settle(2, slot, R3.at[slot])
        for h in range(2):
            q = spots[h][1]
            after, before = wrap(q + 1), wrap(q + side - 1)
            SB[slot % SENT, h, 0, 0:2] = (ACC[slot, h, after, 0:2] + R3[slot, h, 0:2].astype(F32)).astype(BF16)
            SB[slot % SENT, h, 0, 2:3] = ACC[slot, h, after, 2:3].astype(BF16)
            SB[slot % SENT, h, 1, 0:2] = ACC[slot, h, before, 0:2].astype(BF16)
            SB[slot % SENT, h, 1, 2:3] = (ACC[slot, h, before, 2:3] + R3[slot, h, 2:3].astype(F32)).astype(BF16)
            both(3, slot, h)

    def by_layer(c, do):
        for l in range(2):
            pl.when(c // nb == 1 - l)(functools.partial(do, l))

    def gather_message(part, l, slot, h, way, c):
        q, to_q = spots[h][1], spots[h][3]
        step = 1 - 2 * way
        at = q if part < 2 else wrap(q + side - step)
        dst = set_gu[l][h].at[at, c % nb] if part % 2 == 0 else set_d[h].at[at, c]
        src = (OWN.at[slot % SENT, h, pl.ds(0, 2)] if part == 0 else OWN.at[slot % SENT, h, 2]) if part < 2 else dst
        return remote(src, dst, 4 + part // 2, slot, to_q(step))

    def own_copy(part, l, slot, h, c):
        q = spots[h][1]
        if part == 0:
            return pltpu.make_async_copy(OWN.at[slot % SENT, h, pl.ds(0, 2)], set_gu[l][h].at[q, c % nb], own_sems.at[slot])
        return pltpu.make_async_copy(OWN.at[slot % SENT, h, 2], set_d[h].at[q, c], own_sems.at[slot])

    def stage4(c):
        slot = c % SLOTS
        settle(3, slot, R4.at[slot])
        for h in range(2):
            q = spots[h][1]
            g = (ACC[slot, h, q] + R4[slot, h, 0].astype(F32) + R4[slot, h, 1].astype(F32)).astype(BF16)
            OWN[slot % SENT, h] = g
            g = g.astype(F32)
            SQ[...] += g[0] * g[0] + g[1] * g[1] + g[2] * g[2]

            def gate_up(l, h=h):
                own_copy(0, l, slot, h, c).start()
                for way in range(2):
                    gather_message(0, l, slot, h, way, c).start()

            by_layer(c, gate_up)
            own_copy(1, 0, slot, h, c).start()
            for way in range(2):
                gather_message(1, 0, slot, h, way, c).start()

    def stage5(c):
        slot = c % SLOTS
        settle(4, slot, R4.at[slot])
        pltpu.make_async_copy(R3.at[slot], R3.at[slot], own_sems.at[slot]).wait()
        for h in range(2):
            by_layer(c, lambda l, h=h: gather_message(2, l, slot, h, 1, c).start())
            gather_message(3, 0, slot, h, 0, c).start()

    def stage6(c):
        slot = c % SLOTS
        settle(5, slot, R3.at[slot])

    def square(d):
        return pltpu.make_async_remote_copy(
            src_ref=MINE, dst_ref=SQS.at[me], send_sem=sq_sems.at[0, d], recv_sem=sq_sems.at[1, d],
            device_id={"dp": lax.rem(me + d, n)}, device_id_type=MESH,
        )

    def squares():
        total = jnp.broadcast_to(jnp.sum(SQ[...], axis=0, keepdims=True), MINE.shape)
        MINE[...] = total
        SQS[me] = total
        for d in range(1, n):
            square(d).start()

    def load(which, l=1):
        src, dst = {"A": (a_hbm.at[l], A), "AT": (at_hbm.at[l], AT), "H": (h_hbm, H), "DY": (dy_hbm.at[0], DY), "DYT": (dyt_hbm, DYT),
                    "WG1": (wg_hbm.at[1], WG1), "WU1": (wu_hbm.at[1], WU1)}[which]
        return pltpu.make_async_copy(src, dst, load_sems.at[("A", "AT", "H", "DY", "DYT", "WG1", "WU1").index(which)])

    def weights(i, what):
        l, at, slot = 1 - i // nb, pl.multiple_of((i % nb) * BLOCK, BLOCK), i % 2
        for j, (src, dst) in enumerate((
            (wg_hbm.at[l, :, pl.ds(at, BLOCK)], WB.at[slot, 0]),
            (wu_hbm.at[l, :, pl.ds(at, BLOCK)], WB.at[slot, 1]),
            (wd_hbm.at[l, pl.ds(at, BLOCK), :], WD.at[slot]),
        )):
            getattr(pltpu.make_async_copy(src, dst, w_sems.at[slot, j]), what)()

    def middle():
        load("A", 0).start()
        load("AT", 0).start()
        for which in ("H", "WG1", "WU1"):
            load(which).wait()
        for t in range(tokens // rows):
            at = slice(t * rows, (t + 1) * rows)
            by_a = dot(DG[at, :], WG1[...], ((1,), (1,))).astype(BF16).astype(F32)
            by_a = (by_a + dot(DU[at, :], WU1[...], ((1,), (1,))).astype(BF16).astype(F32)).astype(BF16).astype(F32)
            wide = H[at, :].astype(F32)
            scale = lax.rsqrt(jnp.mean(wide * wide, -1, keepdims=True) + 1e-6)
            by_scale = jnp.sum(by_a * wide, -1, keepdims=True)
            by_wide = (by_a * scale - wide * (by_scale * scale * scale * scale * (1.0 / d))).astype(BF16).astype(F32)
            by_h = (DY[at, :].astype(F32) + by_wide).astype(BF16)
            DY[at, :] = by_h
            DYT[:, at] = by_h.T
        load("A", 0).wait()
        load("AT", 0).wait()

    def compute(i):
        slot, ws = i % SLOTS, i % 2
        cols = pl.ds(pl.multiple_of((i % nb) * BLOCK, BLOCK), BLOCK)
        weights(i, "wait")

        @pl.when(i + 1 < chunks)
        def _():
            weights(i + 1, "start")

        for t in range(tokens // rows):
            at = slice(t * rows, (t + 1) * rows)
            gate, up = dot(A[at, :], WB[ws, 0]), dot(A[at, :], WB[ws, 1])
            by_act = dot(DY[at, :], WD[ws], ((1,), (1,))).astype(BF16).astype(F32)
            sig = sigmoid(gate)
            silu = gate * sig
            ACT[at, :] = (silu * up).astype(BF16)
            DU[at, cols] = (by_act * silu).astype(BF16)
            DG[at, cols] = (by_act * up * (sig * (1.0 + gate * (1.0 - sig)))).astype(BF16)

        @pl.when(i == 0)
        def _():
            load("AT").wait()
            load("DYT").wait()

        for j, (left, right) in enumerate(((AT, DG[:, cols]), (AT, DU[:, cols]), (DYT, ACT[...]))):
            g = dot(left[...], right)
            for o in range(2 * side):
                piece = g[o * side * pr : (o + 1) * side * pr].reshape(side, pr, BLOCK)
                TERM[slot, o // side, o % side, :, j] = piece.astype(BF16)

    for which in ("A", "DY", "AT", "DYT", "H", "WG1", "WU1"):
        load(which).start()
    weights(0, "start")
    barrier = pltpu.get_barrier_semaphore()
    for other in range(1, n):
        pl.semaphore_signal(barrier, inc=1, device_id={"dp": lax.rem(me + other, n)}, device_id_type=MESH)
    SQ[...] = jnp.zeros_like(SQ)
    load("A").wait()
    load("DY").wait()
    pl.semaphore_wait(barrier, n - 1)

    @pl.loop(0, chunks + 6 * LAG)
    def _(i):
        pl.when(i == nb)(middle)
        pl.when(i < chunks)(lambda: compute(i))
        pl.when(i < chunks)(lambda: stage0(i))
        for lag, stage in enumerate((stage1, stage2, stage3, stage4, stage5, stage6), 1):
            late = lag * LAG
            pl.when((i >= late) & (i < chunks + late))(functools.partial(stage, i - late))
        pl.when(i == chunks - 1 + 4 * LAG)(squares)

    for other in range(1, n):
        square(other).wait_recv()
    for other in range(1, n):
        square(other).wait_send()
    total = jnp.zeros(MINE.shape, F32)
    for device in range(n):
        total = total + SQS[device]
    total = jnp.sum(total[0:1], axis=1, keepdims=True)
    f_ref[...] = jnp.broadcast_to(jnp.minimum(1.0, 0.5 * lax.rsqrt(total / count + 1e-30)), f_ref.shape)


def backward(side, count, a, at, h, dy, dyt, wg, wu, wd):
    _, tokens, d = a.shape
    ff = wg.shape[2]
    nb = ff // BLOCK
    pr = d // (2 * side**2)
    piece = (3, pr, BLOCK)
    v = pltpu.VMEM
    sems = pltpu.SemaphoreType.DMA
    shapes = [(side, 2 * nb, pr, BLOCK)] * 2 + [(side, nb, 2, pr, BLOCK)] * 4
    out = pl.pallas_call(
        functools.partial(backward_kernel, side, count),
        out_shape=[jax.ShapeDtypeStruct(s, BF16) for s in shapes] + [jax.ShapeDtypeStruct((8, LANES), F32)],
        in_specs=[ANY] * 8,
        out_specs=[ANY] * 6 + [VMEM],
        scratch_shapes=[
            v((tokens, d), BF16), v((d, tokens), BF16), v((tokens, d), BF16), v((tokens, d), BF16), v((d, tokens), BF16),
            v((tokens, BLOCK), BF16), v((tokens, ff), BF16), v((tokens, ff), BF16),
            v((2, 2, d, BLOCK), BF16), v((2, BLOCK, d), BF16), v((d, ff), BF16), v((d, ff), BF16),
            v((SLOTS, 2, side, side, *piece), BF16), v((SLOTS, 2, 2, 2, *piece), BF16), v((SLOTS, 2, 2, side, *piece), BF16),
            v((SLOTS, 2, *piece), BF16), v((SLOTS, 2, 2, *piece), BF16), v((SLOTS, 2, side, *piece), F32),
            v((SENT, 2, *piece), BF16), v((SENT, 2, 2, *piece), BF16), v((SENT, 2, *piece), BF16),
            v((pr, BLOCK), F32), v((8, BLOCK), F32), v((side**2, 8, BLOCK), F32),
            sems((7,)), sems((2, 3)), sems((6, SLOTS)), sems((6, SLOTS)), sems((SLOTS,)), sems((2, side**2)),
        ],
        compiler_params=pltpu.CompilerParams(collective_id=0, has_side_effects=True, vmem_limit_bytes=67043328),
        cost_estimate=pl.CostEstimate(flops=28 * tokens * d * ff, bytes_accessed=2 * (7 * tokens * d + 8 * d * ff), transcendentals=2 * tokens * ff),
        name="backward",
    )(a, at, h, dy, dyt, wg, wu, wd)
    return out[0:2], (out[2:4], out[4:6]), out[6]


def adamw(f, g, w, m, v):
    g = g.astype(F32) * f
    m = 0.9 * m + 0.1 * g
    v = 0.95 * v + 0.05 * g * g
    w = w.astype(F32)
    return (w - 0.02 * (m * lax.rsqrt(v + 1e-8) + 0.1 * w)).astype(BF16), m, v


STEP = 4


def wide_kernel(count, table, f_ref, *refs):
    parts, ins, outs = refs[:count], refs[count : count + 6], refs[-6:]
    f = f_ref[0:1, 0:1]
    per = 4 // STEP
    step = pl.program_id(0)
    for s in range(count):

        @pl.when(step // per == s)
        def _(part=parts[s]):
            _, nb, _, pr, _ = part.shape

            @pl.loop(0, nb)
            def _(b):
                cols = pl.ds(pl.multiple_of(b * BLOCK, BLOCK), BLOCK)
                for j in range(2):
                    w, m, v = ins[j::2]
                    nw, nm, nv = outs[j::2]
                    for q in range(STEP):
                        at = slice(q * pr, (q + 1) * pr)
                        nw[0, at, cols], nm[0, at, cols], nv[0, at, cols] = adamw(f, part[q, b, j], w[0, at, cols], m[0, at, cols], v[0, at, cols])


def update_wide(table, f, parts, arrays, before):
    _, _, ff = arrays[0].shape
    side, _, _, pr, _ = parts[0][0].shape
    per = side // STEP

    def pick(i, values):
        which, chosen = i // per, values[-1]
        for s in range(len(values) - 2, -1, -1):
            chosen = jnp.where(which == s, values[s], chosen)
        return chosen

    layers, indices = [l for _, l, _ in parts], [index for _, _, index in parts]
    block = pl.BlockSpec((1, STEP * pr, ff), lambda i, table: (pick(i, layers), table[pick(i, indices)] * per + i % per, 0))

    def part_spec(s):
        shape = parts[s][0].shape
        return pl.BlockSpec((STEP, *shape[1:]), lambda i, table: (jnp.clip(i - s * per, 0, per - 1), 0, 0, 0, 0))

    size = 2 * len(parts) * side * pr * ff
    return pl.pallas_call(
        functools.partial(wide_kernel, len(parts)),
        grid_spec=pltpu.PrefetchScalarGridSpec(
            num_scalar_prefetch=1,
            grid=(len(parts) * per,),
            in_specs=[pl.BlockSpec((8, LANES), lambda i, table: (0, 0))] + [part_spec(s) for s in range(len(parts))] + [block] * 6 + [ANY] * len(before),
            out_specs=[block] * 6,
        ),
        out_shape=[jax.ShapeDtypeStruct(a.shape, a.dtype) for a in arrays],
        input_output_aliases={2 + len(parts) + 6 + i: i for i in range(len(before))},
        compiler_params=pltpu.CompilerParams(vmem_limit_bytes=62 * 2**20),
        cost_estimate=pl.CostEstimate(flops=1000 * size, bytes_accessed=22 * size, transcendentals=size),
        name="update_wide",
    )(table, f, *(g for g, _, _ in parts), *arrays, *before)


def tall_kernel(indices, table, f_ref, *refs):
    count = len(indices)
    parts, (w, m, v, nw, nm, nv, whole) = refs[:count], refs[count:]
    f = f_ref[0:1, 0:1]
    for s, part in enumerate(parts):
        rows = part.shape[0] * part.shape[2]
        index, first = indices[s]
        whole[pl.ds(pl.multiple_of(table[index] * (4 * part.shape[2]) + first * part.shape[2], 8), rows), :] = part[:, 0].astype(F32).reshape(rows, BLOCK)
    for at in range(0, BLOCK, LANES):
        rows = slice(at, at + LANES)
        g = whole[:, rows].T
        nw[0, rows, :], nm[0, rows, :], nv[0, rows, :] = adamw(f, g, w[0, rows, :], m[0, rows, :], v[0, rows, :])


def update_tall(table, f, parts, w, m, v):
    layers, ff, d = w.shape
    nb = ff // BLOCK
    block = pl.BlockSpec((1, BLOCK, d), lambda c, table: (layers - 1 - c // nb, c % nb, 0))
    size = layers * d * ff
    return pl.pallas_call(
        functools.partial(tall_kernel, [(index, first) for _, index, first in parts]),
        grid_spec=pltpu.PrefetchScalarGridSpec(
            num_scalar_prefetch=1,
            grid=(layers * nb,),
            in_specs=[pl.BlockSpec((8, LANES), lambda c, table: (0, 0))]
            + [pl.BlockSpec((g.shape[0], 1, *g.shape[2:]), lambda c, table: (0, c, 0, 0)) for g, _, _ in parts]
            + [block] * 3,
            out_specs=[block] * 3,
            scratch_shapes=[pltpu.VMEM((d, BLOCK), F32)],
        ),
        out_shape=[jax.ShapeDtypeStruct(a.shape, a.dtype) for a in (w, m, v)],
        compiler_params=pltpu.CompilerParams(vmem_limit_bytes=62 * 2**20),
        cost_estimate=pl.CostEstimate(flops=1000 * size, bytes_accessed=22 * size, transcendentals=size),
        name="update_tall",
    )(table, f, *(g for g, _, _ in parts), w, m, v)


def solution(mesh):
    n = mesh.shape["dp"]
    side = math.isqrt(n)
    along = lambda h, i, step: ((i // side + step) % side) * side + i % side if h == 0 else i // side * side + (i + step) % side

    def move(array, h, step):
        return lax.ppermute(array, "dp", [(i, along(h, i, step)) for i in range(n)])

    def near(sets):
        return [move(mine, h, to) for h, mine in enumerate(sets) for to in (1, -1)]

    def halves(sets):
        return [part[: side // 2] if i % 2 == 0 else part[side // 2 :] for i, part in enumerate(sets)]

    def far(parts):
        return [move(part, i // 2, 1 - 2 * (i % 2)) for i, part in enumerate(parts)]

    def step(x, dy, wg, wu, wd, mg, mu, md, vg, vu, vd):
        a, at, h, dyt = forward(x, dy, wg, wu, wd)
        set_d, set_gu, f = backward(side, float(wg.size + wu.size + wd.size), a, at, h, dy, dyt, wg, wu, wd)
        p = [spot[0] for spot in places(side)]
        table = [h * side + p[h] for h in range(2)]
        table += [h * side + (p[h] + side - to) % side for h in range(2) for to in (1, -1)]
        table += [h * side + (p[h] + 2) % side for h in range(2)]
        table = jnp.stack(table).astype(jnp.int32)
        arrays = (wg, wu, mg, mu, vg, vu)
        wide = lambda parts, before: update_wide(table, f, parts, arrays, before)

        near_d = near(set_d)
        new = wide([(set_gu[1][h], 1, h) for h in range(2)], ())
        half_d, new = lax.optimization_barrier((halves(near_d), new))
        far_d = far(half_d)
        new = wide([(set_gu[0][h], 0, h) for h in range(2)], new)
        far_d, set_gu, new = lax.optimization_barrier((far_d, set_gu, new))
        near_gu = {l: near(set_gu[l]) for l in (1, 0)}
        parts = [(set_d[h], h, 0) for h in range(2)] + [(g, 2 + i, 0) for i, g in enumerate(near_d)]
        parts += [(g, 6 + i // 2, (i % 2) * (side // 2)) for i, g in enumerate(far_d)]
        tall = update_tall(table, f, parts, wd, md, vd)
        near_gu, tall, new = lax.optimization_barrier((near_gu, tall, new))
        far_gu = [(move(near_gu[l][2 * h + 1 - l], h, 2 * l - 1), l, 6 + h) for l in (1, 0) for h in range(2)]
        new = wide([(g, l, 2 + i) for l in (1, 0) for i, g in enumerate(near_gu[l])], new)
        new = wide(far_gu, new)
        return new[0], new[1], tall[0], new[2], new[3], tall[1], new[4], new[5], tall[2]

    return jax.shard_map(
        step,
        mesh=mesh,
        in_specs=(P(("rep", "dp"), None, None),) * 2 + (P(None, None, None),) * 9,
        out_specs=(P("rep", None, None),) * 9,
        check_vma=False,
    )
```

```python
import functools
import math

import jax
import jax.numpy as jnp
from jax import lax
from jax.experimental import pallas as pl
from jax.experimental.pallas import tpu as pltpu
from jax.sharding import PartitionSpec as P

MESH = pl.DeviceIdType.MESH
BLOCK = 256
LANES = 128
LAG = 2
SLOTS = 2 * LAG + 2
SENT = LAG + 1
BF16, F32 = jnp.bfloat16, jnp.float32
ANY = pl.BlockSpec(memory_space=pl.ANY)
VMEM = pl.BlockSpec(memory_space=pltpu.VMEM)


def dot(a, b, over=((1,), (0,))):
    return lax.dot_general(a, b, (over, ((), ())), preferred_element_type=F32)


def sigmoid(v):
    return 0.5 + 0.5 * jnp.tanh(0.5 * v)


def normed(wide):
    return (wide * lax.rsqrt(jnp.mean(wide * wide, -1, keepdims=True) + 1e-6)).astype(BF16)


def forward_kernel(x_ref, dy_ref, wg_ref, wu_ref, wd_ref, a_ref, at_ref, h_ref, dyt_ref, act):
    rows = x_ref.shape[1] // 2
    for t in range(2):
        at = slice(t * rows, (t + 1) * rows)
        x = x_ref[0, at].astype(F32)
        a = normed(x)
        a_ref[0, at] = a
        at_ref[0, :, at] = a.T
        for b in range(wg_ref.shape[2] // BLOCK):
            cols = slice(b * BLOCK, (b + 1) * BLOCK)
            gate, up = dot(a, wg_ref[0, :, cols]), dot(a, wu_ref[0, :, cols])
            act[at, cols] = (gate * sigmoid(gate) * up).astype(BF16)
        dyt_ref[:, at] = dy_ref[0, at].T
        h = (x + dot(act[at, :], wd_ref[0]).astype(BF16).astype(F32)).astype(BF16)
        h_ref[at, :] = h
        a = normed(h.astype(F32))
        a_ref[1, at] = a
        at_ref[1, :, at] = a.T


def forward(x, dy, wg, wu, wd):
    _, tokens, d = x.shape
    ff = wg.shape[2]
    rows = min(512, tokens)
    tall = pl.BlockSpec((1, rows, d), lambda i: (0, i, 0))
    out = [((2, tokens, d), (2, rows, d), lambda i: (0, i, 0)), ((2, d, tokens), (2, d, rows), lambda i: (0, 0, i))]
    out += [((tokens, d), (rows, d), lambda i: (i, 0)), ((d, tokens), (d, rows), lambda i: (0, i))]
    return pl.pallas_call(
        forward_kernel,
        grid=(tokens // rows,),
        out_shape=[jax.ShapeDtypeStruct(s, BF16) for s, _, _ in out],
        in_specs=[tall, tall]
        + [pl.BlockSpec((1, *w.shape[1:]), lambda i: (0, 0, 0), pipeline_mode=pl.Buffered(1)) for w in (wg, wu, wd)],
        out_specs=[pl.BlockSpec(b, m) for _, b, m in out],
        scratch_shapes=[pltpu.VMEM((rows, ff), BF16)],
        compiler_params=pltpu.CompilerParams(vmem_limit_bytes=60 * 2**20),
        cost_estimate=pl.CostEstimate(flops=6 * tokens * d * ff, bytes_accessed=2 * (9 * tokens * d + 3 * d * ff), transcendentals=tokens * ff),
        name="forward",
    )(x, dy, wg, wu, wd)


def places(side):
    me = lax.axis_index("dp")
    x, y = me // side, me % side
    along_x = lambda d: lax.rem(x + side + d, side) * side + y
    along_y = lambda d: x * side + lax.rem(y + side + d, side)
    return ((x, y, along_x, along_y), (y, x, along_y, along_x))


def backward_kernel(side, count, a_hbm, at_hbm, h_hbm, dy_hbm, dyt_hbm, wg_hbm, wu_hbm, wd_hbm, *refs):
    set_d, set_gu, f_ref, scratch = refs[0:2], (refs[2:4], refs[4:6]), refs[6], refs[7:]
    (A, AT, H, DY, DYT, ACT, DG, DU, WB, WD, WG1, WU1, TERM, R1, R2, R3, R4, ACC, SA, SB, OWN, SQ, MINE, SQS) = scratch[:-6]
    load_sems, w_sems, send_sems, recv_sems, own_sems, sq_sems = scratch[-6:]
    tokens, d = A.shape
    ff = DG.shape[1]
    nb = ff // BLOCK
    chunks = 2 * nb
    rows = min(512, tokens)
    n = side * side
    me = lax.axis_index("dp")
    pr = d // (2 * n)
    spots = places(side)
    wrap = lambda v: lax.rem(v, side)

    def remote(src, dst, stage, slot, to):
        return pltpu.make_async_remote_copy(
            src_ref=src, dst_ref=dst, send_sem=send_sems.at[stage, slot], recv_sem=recv_sems.at[stage, slot],
            device_id={"dp": to}, device_id_type=MESH,
        )

    def settle(stage, slot, like):
        copy = remote(like, like, stage, slot, me)
        copy.wait_recv()
        copy.wait_send()

    def message(stage, slot, h, way):
        p, q, to_p, to_q = spots[h]
        step = 1 - 2 * way
        if stage == 0:
            return remote(TERM.at[slot, h, wrap(p + 2), pl.ds(2 * way, 2)], R1.at[slot, h, way], 0, slot, to_p(step))
        if stage == 1:
            return remote(TERM.at[slot, h, wrap(p + side + step)], R2.at[slot, h, way], 1, slot, to_p(step))
        if stage == 2:
            part = pl.ds(2 * way, 2 - way)
            return remote(SA.at[slot % SENT, h, part], R3.at[slot, h, part], 2, slot, to_q(step))
        return remote(SB.at[slot % SENT, h, way], R4.at[slot, h, way], 3, slot, to_q(step))

    def both(stage, slot, h):
        for way in range(2):
            message(stage, slot, h, way).start()

    def stage0(c):
        for h in range(2):
            both(0, c % SLOTS, h)

    def stage1(c):
        slot = c % SLOTS
        settle(0, slot, R1.at[slot])
        for h in range(2):
            p = spots[h][0]
            for way, at in ((0, wrap(p + 1)), (1, wrap(p + side - 1))):
                half = pl.ds(2 * way, 2)
                TERM[slot, h, at, half] = (TERM[slot, h, at, half].astype(F32) + R1[slot, h, way].astype(F32)).astype(BF16)
            both(1, slot, h)

    def stage2(c):
        slot = c % SLOTS
        settle(1, slot, R2.at[slot])
        for h in range(2):
            p, q = spots[h][:2]
            for o in range(side):
                ACC[slot, h, o] = TERM[slot, h, p, o].astype(F32) + R2[slot, h, 0, o].astype(F32) + R2[slot, h, 1, o].astype(F32)
            SA[slot % SENT, h] = ACC[slot, h, wrap(q + 2)].astype(BF16)
            both(2, slot, h)

    def stage3(c):
        slot = c % SLOTS
        settle(2, slot, R3.at[slot])
        for h in range(2):
            q = spots[h][1]
            after, before = wrap(q + 1), wrap(q + side - 1)
            SB[slot % SENT, h, 0, 0:2] = (ACC[slot, h, after, 0:2] + R3[slot, h, 0:2].astype(F32)).astype(BF16)
            SB[slot % SENT, h, 0, 2:3] = ACC[slot, h, after, 2:3].astype(BF16)
            SB[slot % SENT, h, 1, 0:2] = ACC[slot, h, before, 0:2].astype(BF16)
            SB[slot % SENT, h, 1, 2:3] = (ACC[slot, h, before, 2:3] + R3[slot, h, 2:3].astype(F32)).astype(BF16)
            both(3, slot, h)

    def by_layer(c, do):
        for l in range(2):
            pl.when(c // nb == 1 - l)(functools.partial(do, l))

    def gather_message(part, l, slot, h, way, c):
        q, to_q = spots[h][1], spots[h][3]
        step = 1 - 2 * way
        at = q if part < 2 else wrap(q + side - step)
        dst = set_gu[l][h].at[at, c % nb] if part % 2 == 0 else set_d[h].at[at, c]
        src = (OWN.at[slot % SENT, h, pl.ds(0, 2)] if part == 0 else OWN.at[slot % SENT, h, 2]) if part < 2 else dst
        return remote(src, dst, 4 + part // 2, slot, to_q(step))

    def own_copy(part, l, slot, h, c):
        q = spots[h][1]
        if part == 0:
            return pltpu.make_async_copy(OWN.at[slot % SENT, h, pl.ds(0, 2)], set_gu[l][h].at[q, c % nb], own_sems.at[slot])
        return pltpu.make_async_copy(OWN.at[slot % SENT, h, 2], set_d[h].at[q, c], own_sems.at[slot])

    def stage4(c):
        slot = c % SLOTS
        settle(3, slot, R4.at[slot])
        for h in range(2):
            q = spots[h][1]
            g = (ACC[slot, h, q] + R4[slot, h, 0].astype(F32) + R4[slot, h, 1].astype(F32)).astype(BF16)
            OWN[slot % SENT, h] = g
            g = g.astype(F32)
            SQ[...] += g[0] * g[0] + g[1] * g[1] + g[2] * g[2]

            def gate_up(l, h=h):
                own_copy(0, l, slot, h, c).start()
                for way in range(2):
                    gather_message(0, l, slot, h, way, c).start()

            by_layer(c, gate_up)
            own_copy(1, 0, slot, h, c).start()
            for way in range(2):
                gather_message(1, 0, slot, h, way, c).start()

    def stage5(c):
        slot = c % SLOTS
        settle(4, slot, R4.at[slot])
        pltpu.make_async_copy(R3.at[slot], R3.at[slot], own_sems.at[slot]).wait()
        for h in range(2):
            by_layer(c, lambda l, h=h: gather_message(2, l, slot, h, 1, c).start())
            gather_message(3, 0, slot, h, 0, c).start()

    def stage6(c):
        slot = c % SLOTS
        settle(5, slot, R3.at[slot])

    def square(d):
        return pltpu.make_async_remote_copy(
            src_ref=MINE, dst_ref=SQS.at[me], send_sem=sq_sems.at[0, d], recv_sem=sq_sems.at[1, d],
            device_id={"dp": lax.rem(me + d, n)}, device_id_type=MESH,
        )

    def squares():
        total = jnp.broadcast_to(jnp.sum(SQ[...], axis=0, keepdims=True), MINE.shape)
        MINE[...] = total
        SQS[me] = total
        for d in range(1, n):
            square(d).start()

    def load(which, l=1):
        src, dst = {"A": (a_hbm.at[l], A), "AT": (at_hbm.at[l], AT), "H": (h_hbm, H), "DY": (dy_hbm.at[0], DY), "DYT": (dyt_hbm, DYT),
                    "WG1": (wg_hbm.at[1], WG1), "WU1": (wu_hbm.at[1], WU1)}[which]
        return pltpu.make_async_copy(src, dst, load_sems.at[("A", "AT", "H", "DY", "DYT", "WG1", "WU1").index(which)])

    def weights(i, what):
        l, at, slot = 1 - i // nb, pl.multiple_of((i % nb) * BLOCK, BLOCK), i % 2
        for j, (src, dst) in enumerate((
            (wg_hbm.at[l, :, pl.ds(at, BLOCK)], WB.at[slot, 0]),
            (wu_hbm.at[l, :, pl.ds(at, BLOCK)], WB.at[slot, 1]),
            (wd_hbm.at[l, pl.ds(at, BLOCK), :], WD.at[slot]),
        )):
            getattr(pltpu.make_async_copy(src, dst, w_sems.at[slot, j]), what)()

    def middle():
        load("A", 0).start()
        load("AT", 0).start()
        for which in ("H", "WG1", "WU1"):
            load(which).wait()
        for t in range(tokens // rows):
            at = slice(t * rows, (t + 1) * rows)
            by_a = dot(DG[at, :], WG1[...], ((1,), (1,))).astype(BF16).astype(F32)
            by_a = (by_a + dot(DU[at, :], WU1[...], ((1,), (1,))).astype(BF16).astype(F32)).astype(BF16).astype(F32)
            wide = H[at, :].astype(F32)
            scale = lax.rsqrt(jnp.mean(wide * wide, -1, keepdims=True) + 1e-6)
            by_scale = jnp.sum(by_a * wide, -1, keepdims=True)
            by_wide = (by_a * scale - wide * (by_scale * scale * scale * scale * (1.0 / d))).astype(BF16).astype(F32)
            by_h = (DY[at, :].astype(F32) + by_wide).astype(BF16)
            DY[at, :] = by_h
            DYT[:, at] = by_h.T
        load("A", 0).wait()
        load("AT", 0).wait()

    def compute(i):
        slot, ws = i % SLOTS, i % 2
        cols = pl.ds(pl.multiple_of((i % nb) * BLOCK, BLOCK), BLOCK)
        weights(i, "wait")

        @pl.when(i + 1 < chunks)
        def _():
            weights(i + 1, "start")

        for t in range(tokens // rows):
            at = slice(t * rows, (t + 1) * rows)
            gate, up = dot(A[at, :], WB[ws, 0]), dot(A[at, :], WB[ws, 1])
            by_act = dot(DY[at, :], WD[ws], ((1,), (1,))).astype(BF16).astype(F32)
            sig = sigmoid(gate)
            silu = gate * sig
            ACT[at, :] = (silu * up).astype(BF16)
            DU[at, cols] = (by_act * silu).astype(BF16)
            DG[at, cols] = (by_act * up * (sig * (1.0 + gate * (1.0 - sig)))).astype(BF16)

        @pl.when(i == 0)
        def _():
            load("AT").wait()
            load("DYT").wait()

        for j, (left, right) in enumerate(((AT, DG[:, cols]), (AT, DU[:, cols]), (DYT, ACT[...]))):
            g = dot(left[...], right)
            for o in range(2 * side):
                piece = g[o * side * pr : (o + 1) * side * pr].reshape(side, pr, BLOCK)
                TERM[slot, o // side, o % side, :, j] = piece.astype(BF16)

    for which in ("A", "DY", "AT", "DYT", "H", "WG1", "WU1"):
        load(which).start()
    weights(0, "start")
    barrier = pltpu.get_barrier_semaphore()
    for other in range(1, n):
        pl.semaphore_signal(barrier, inc=1, device_id={"dp": lax.rem(me + other, n)}, device_id_type=MESH)
    SQ[...] = jnp.zeros_like(SQ)
    load("A").wait()
    load("DY").wait()
    pl.semaphore_wait(barrier, n - 1)

    def first(c):
        compute(c)
        stage0(c)

    @pl.loop(0, chunks + 1 + 6 * LAG)
    def _(i):
        pl.when(i == nb)(middle)
        for lag, stage in enumerate((first, stage1, stage2, stage3, stage4, stage5, stage6)):
            at = i - lag * LAG
            pl.when((at >= 0) & (at != nb) & (at <= chunks))(functools.partial(stage, at - jnp.where(at > nb, 1, 0)))
        pl.when(i == chunks + 4 * LAG)(squares)

    for other in range(1, n):
        square(other).wait_recv()
    for other in range(1, n):
        square(other).wait_send()
    total = jnp.zeros(MINE.shape, F32)
    for device in range(n):
        total = total + SQS[device]
    total = jnp.sum(total[0:1], axis=1, keepdims=True)
    f_ref[...] = jnp.broadcast_to(jnp.minimum(1.0, 0.5 * lax.rsqrt(total / count + 1e-30)), f_ref.shape)


def backward(side, count, a, at, h, dy, dyt, wg, wu, wd):
    _, tokens, d = a.shape
    ff = wg.shape[2]
    nb = ff // BLOCK
    pr = d // (2 * side**2)
    piece = (3, pr, BLOCK)
    v = pltpu.VMEM
    sems = pltpu.SemaphoreType.DMA
    shapes = [(side, 2 * nb, pr, BLOCK)] * 2 + [(side, nb, 2, pr, BLOCK)] * 4
    out = pl.pallas_call(
        functools.partial(backward_kernel, side, count),
        out_shape=[jax.ShapeDtypeStruct(s, BF16) for s in shapes] + [jax.ShapeDtypeStruct((8, LANES), F32)],
        in_specs=[ANY] * 8,
        out_specs=[ANY] * 6 + [VMEM],
        scratch_shapes=[
            v((tokens, d), BF16), v((d, tokens), BF16), v((tokens, d), BF16), v((tokens, d), BF16), v((d, tokens), BF16),
            v((tokens, BLOCK), BF16), v((tokens, ff), BF16), v((tokens, ff), BF16),
            v((2, 2, d, BLOCK), BF16), v((2, BLOCK, d), BF16), v((d, ff), BF16), v((d, ff), BF16),
            v((SLOTS, 2, side, side, *piece), BF16), v((SLOTS, 2, 2, 2, *piece), BF16), v((SLOTS, 2, 2, side, *piece), BF16),
            v((SLOTS, 2, *piece), BF16), v((SLOTS, 2, 2, *piece), BF16), v((SLOTS, 2, side, *piece), F32),
            v((SENT, 2, *piece), BF16), v((SENT, 2, 2, *piece), BF16), v((SENT, 2, *piece), BF16),
            v((pr, BLOCK), F32), v((8, BLOCK), F32), v((side**2, 8, BLOCK), F32),
            sems((7,)), sems((2, 3)), sems((6, SLOTS)), sems((6, SLOTS)), sems((SLOTS,)), sems((2, side**2)),
        ],
        compiler_params=pltpu.CompilerParams(collective_id=0, has_side_effects=True, vmem_limit_bytes=67043328),
        cost_estimate=pl.CostEstimate(flops=28 * tokens * d * ff, bytes_accessed=2 * (7 * tokens * d + 8 * d * ff), transcendentals=2 * tokens * ff),
        name="backward",
    )(a, at, h, dy, dyt, wg, wu, wd)
    return out[0:2], (out[2:4], out[4:6]), out[6]


def adamw(f, g, w, m, v):
    g = g.astype(F32) * f
    m = 0.9 * m + 0.1 * g
    v = 0.95 * v + 0.05 * g * g
    w = w.astype(F32)
    return (w - 0.02 * (m * lax.rsqrt(v + 1e-8) + 0.1 * w)).astype(BF16), m, v


STEP = 4


def wide_kernel(count, table, f_ref, *refs):
    parts, ins, outs = refs[:count], refs[count : count + 6], refs[-6:]
    f = f_ref[0:1, 0:1]
    per = 4 // STEP
    step = pl.program_id(0)
    for s in range(count):

        @pl.when(step // per == s)
        def _(part=parts[s]):
            _, nb, _, pr, _ = part.shape

            @pl.loop(0, nb)
            def _(b):
                cols = pl.ds(pl.multiple_of(b * BLOCK, BLOCK), BLOCK)
                for j in range(2):
                    w, m, v = ins[j::2]
                    nw, nm, nv = outs[j::2]
                    for q in range(STEP):
                        at = slice(q * pr, (q + 1) * pr)
                        nw[0, at, cols], nm[0, at, cols], nv[0, at, cols] = adamw(f, part[q, b, j], w[0, at, cols], m[0, at, cols], v[0, at, cols])


def update_wide(table, f, parts, arrays, before):
    _, _, ff = arrays[0].shape
    side, _, _, pr, _ = parts[0][0].shape
    per = side // STEP

    def pick(i, values):
        which, chosen = i // per, values[-1]
        for s in range(len(values) - 2, -1, -1):
            chosen = jnp.where(which == s, values[s], chosen)
        return chosen

    layers, indices = [l for _, l, _ in parts], [index for _, _, index in parts]
    block = pl.BlockSpec((1, STEP * pr, ff), lambda i, table: (pick(i, layers), table[pick(i, indices)] * per + i % per, 0))

    def part_spec(s):
        shape = parts[s][0].shape
        return pl.BlockSpec((STEP, *shape[1:]), lambda i, table: (jnp.clip(i - s * per, 0, per - 1), 0, 0, 0, 0))

    size = 2 * len(parts) * side * pr * ff
    return pl.pallas_call(
        functools.partial(wide_kernel, len(parts)),
        grid_spec=pltpu.PrefetchScalarGridSpec(
            num_scalar_prefetch=1,
            grid=(len(parts) * per,),
            in_specs=[pl.BlockSpec((8, LANES), lambda i, table: (0, 0))] + [part_spec(s) for s in range(len(parts))] + [block] * 6 + [ANY] * len(before),
            out_specs=[block] * 6,
        ),
        out_shape=[jax.ShapeDtypeStruct(a.shape, a.dtype) for a in arrays],
        input_output_aliases={2 + len(parts) + 6 + i: i for i in range(len(before))},
        compiler_params=pltpu.CompilerParams(vmem_limit_bytes=62 * 2**20),
        cost_estimate=pl.CostEstimate(flops=1000 * size, bytes_accessed=22 * size, transcendentals=size),
        name="update_wide",
    )(table, f, *(g for g, _, _ in parts), *arrays, *before)


def tall_kernel(indices, table, f_ref, *refs):
    count = len(indices)
    parts, (w, m, v, nw, nm, nv, whole) = refs[:count], refs[count:]
    f = f_ref[0:1, 0:1]
    for s, part in enumerate(parts):
        rows = part.shape[0] * part.shape[2]
        index, first = indices[s]
        whole[pl.ds(pl.multiple_of(table[index] * (4 * part.shape[2]) + first * part.shape[2], 8), rows), :] = part[:, 0].astype(F32).reshape(rows, BLOCK)
    for at in range(0, BLOCK, LANES):
        rows = slice(at, at + LANES)
        g = whole[:, rows].T
        nw[0, rows, :], nm[0, rows, :], nv[0, rows, :] = adamw(f, g, w[0, rows, :], m[0, rows, :], v[0, rows, :])


def update_tall(table, f, parts, w, m, v):
    layers, ff, d = w.shape
    nb = ff // BLOCK
    block = pl.BlockSpec((1, BLOCK, d), lambda c, table: (layers - 1 - c // nb, c % nb, 0))
    size = layers * d * ff
    return pl.pallas_call(
        functools.partial(tall_kernel, [(index, first) for _, index, first in parts]),
        grid_spec=pltpu.PrefetchScalarGridSpec(
            num_scalar_prefetch=1,
            grid=(layers * nb,),
            in_specs=[pl.BlockSpec((8, LANES), lambda c, table: (0, 0))]
            + [pl.BlockSpec((g.shape[0], 1, *g.shape[2:]), lambda c, table: (0, c, 0, 0)) for g, _, _ in parts]
            + [block] * 3,
            out_specs=[block] * 3,
            scratch_shapes=[pltpu.VMEM((d, BLOCK), F32)],
        ),
        out_shape=[jax.ShapeDtypeStruct(a.shape, a.dtype) for a in (w, m, v)],
        compiler_params=pltpu.CompilerParams(vmem_limit_bytes=62 * 2**20),
        cost_estimate=pl.CostEstimate(flops=1000 * size, bytes_accessed=22 * size, transcendentals=size),
        name="update_tall",
    )(table, f, *(g for g, _, _ in parts), w, m, v)


def solution(mesh):
    n = mesh.shape["dp"]
    side = math.isqrt(n)
    along = lambda h, i, step: ((i // side + step) % side) * side + i % side if h == 0 else i // side * side + (i + step) % side

    def move(array, h, step):
        return lax.ppermute(array, "dp", [(i, along(h, i, step)) for i in range(n)])

    def near(sets):
        return [move(mine, h, to) for h, mine in enumerate(sets) for to in (1, -1)]

    def halves(sets):
        return [part[: side // 2] if i % 2 == 0 else part[side // 2 :] for i, part in enumerate(sets)]

    def far(parts):
        return [move(part, i // 2, 1 - 2 * (i % 2)) for i, part in enumerate(parts)]

    def step(x, dy, wg, wu, wd, mg, mu, md, vg, vu, vd):
        a, at, h, dyt = forward(x, dy, wg, wu, wd)
        set_d, set_gu, f = backward(side, float(wg.size + wu.size + wd.size), a, at, h, dy, dyt, wg, wu, wd)
        p = [spot[0] for spot in places(side)]
        table = [h * side + p[h] for h in range(2)]
        table += [h * side + (p[h] + side - to) % side for h in range(2) for to in (1, -1)]
        table += [h * side + (p[h] + 2) % side for h in range(2)]
        table = jnp.stack(table).astype(jnp.int32)
        arrays = (wg, wu, mg, mu, vg, vu)
        wide = lambda parts, before: update_wide(table, f, parts, arrays, before)

        near_d = near(set_d)
        new = wide([(set_gu[1][h], 1, h) for h in range(2)], ())
        half_d, new = lax.optimization_barrier((halves(near_d), new))
        far_d = far(half_d)
        new = wide([(set_gu[0][h], 0, h) for h in range(2)], new)
        far_d, set_gu, new = lax.optimization_barrier((far_d, set_gu, new))
        near_gu = {l: near(set_gu[l]) for l in (1, 0)}
        parts = [(set_d[h], h, 0) for h in range(2)] + [(g, 2 + i, 0) for i, g in enumerate(near_d)]
        parts += [(g, 6 + i // 2, (i % 2) * (side // 2)) for i, g in enumerate(far_d)]
        tall = update_tall(table, f, parts, wd, md, vd)
        near_gu, tall, new = lax.optimization_barrier((near_gu, tall, new))
        far_gu = [(move(near_gu[l][2 * h + 1 - l], h, 2 * l - 1), l, 6 + h) for l in (1, 0) for h in range(2)]
        new = wide([(g, l, 2 + i) for l in (1, 0) for i, g in enumerate(near_gu[l])], new)
        new = wide(far_gu, new)
        return new[0], new[1], tall[0], new[2], new[3], tall[1], new[4], new[5], tall[2]

    return jax.shard_map(
        step,
        mesh=mesh,
        in_specs=(P(("rep", "dp"), None, None),) * 2 + (P(None, None, None),) * 9,
        out_specs=(P("rep", None, None),) * 9,
        check_vma=False,
    )
```
